256 devices in a mesh: samp: 32 (over x, z), feat: 8 (over y, core).
Axes of the slice: x: 4, y: 4, z: 8, core: 2. Of those that a mesh axis runs over, the one named last changes fastest.
Arguments:
- inputs: bfloat16 [65536, 96], P('samp'), may hold values from -6 to 6
- frequencies: bfloat16 [96, 16384], P(None, 'feat'), may hold values from -0.625 to 0.625
- phases: float32 [16384], P('feat'), may hold values from -3.140625 to 3.140625
- targets: float32 [65536], P('samp'), may hold values from -12 to 12
- block_order: int32 [65536], P('samp'), may hold values from 0 to 2047, as said below
Outputs:
- weights: float32 [16384], P('feat')
- duals: float32 [65536], P('samp')
- objectives: float32 [4, 2], replicated
The draws below stay inside these ranges and needn't reach their ends.
Inputs may be any that keep to these rules, and one draw needn't show every extreme that they name: `block_order`: within each aligned run of 2048 samples, a permutation of 0 to 2047.
All inputs are finite; a program needn't handle non-finite values.
Results may differ from the reference program's by a relative error of at most 0.0054.
The reference program's roundings to bfloat16 on the way count: a program that leaves them out, or rounds other values in their place, can miss the bound.
Values may be sent and summed in bfloat16 or wider, within the bound.
A program may use at most 64 MiB of HBM per device.

```python
import math
import jax
import jax.numpy as jnp
from jax import lax

FEATURES = 16384
INPUTS = 96
BLOCK = 256
BLOCKS_DEV = 8
ROUNDS = 4
SAMPLES = 65536
N_SAMP = 32


def draw_targets(key, part):
    index = jnp.arange(SAMPLES, dtype=jnp.float32)
    ramp = 1.0 + 2.0 * index / (SAMPLES - 1)
    base = jnp.clip(jax.random.normal(key, (SAMPLES,), jnp.float32), -4.0, 4.0)
    values = base * ramp
    return values.astype(jnp.float32)


def draw_block_order(key, part):
    row_count = BLOCKS_DEV * BLOCK
    groups = SAMPLES // row_count
    keys = jax.random.split(jax.random.fold_in(key, 7), groups)
    perms = jax.vmap(lambda single: jax.random.permutation(single, row_count))(keys)
    return perms.reshape(SAMPLES).astype(jnp.int32)


def level_of(stream_key, shape, cuts, low, largest):
    loudness = 1.0
    for axis_at, parts in cuts:
        steps = jax.random.uniform(jax.random.fold_in(jax.random.fold_in(stream_key, 6), axis_at), (parts,), jnp.float32, low / len(cuts), largest / len(cuts))
        loudness = loudness * jnp.repeat(jnp.exp(steps), shape[axis_at] // parts).reshape((-1,) + (1,) * (len(shape) - 1 - axis_at))
    return loudness


def noise(key, extent, width, most, pieces=(), kind=jnp.bfloat16):
    loudness = level_of(key, extent, pieces, -0.22, 0.18) if pieces else 1.0
    values = jax.random.normal(key, extent, jnp.float32) * width * loudness
    return jnp.minimum(jnp.maximum(values, -most), most).astype(kind)


def setup_inputs(seed: int = 0) -> dict:
    seeds = jax.random.split(jax.random.key(seed), 6)
    return {
        "inputs": noise(seeds[0], (SAMPLES, INPUTS), 1.0, 6.0, ((0, 32),)),
        "frequencies": noise(seeds[1], (INPUTS, FEATURES), INPUTS ** -0.5, 0.625, ((1, 8),)),
        "phases": jnp.clip(jax.random.uniform(seeds[2], (FEATURES,), jnp.float32, -3.140625, 3.140625), -3.140625, 3.140625),
        "targets": draw_targets(jax.random.fold_in(seeds[5], 71), 0),
        "block_order": draw_block_order(jax.random.fold_in(seeds[5], 71), 0),
    }


highest = lax.Precision.HIGHEST

def feature_block(inputs_part, order_part, frequencies, phases):
    picked = inputs_part[order_part]
    angles = jnp.dot(picked.astype(jnp.float32), frequencies.astype(jnp.float32), precision=highest)
    return (math.sqrt(2.0 / FEATURES) * jnp.cos(angles + phases)).astype(jnp.bfloat16)

def solve_block(factor, vector):
    return jax.scipy.linalg.cho_solve((factor, True), vector)

def reference(inputs, frequencies, phases, targets, block_order):
    row_count = BLOCKS_DEV * BLOCK
    groups = N_SAMP
    ridge = 1.0 / BLOCK
    step_scale = BLOCK / SAMPLES
    inputs_grouped = inputs.reshape(groups, row_count, INPUTS)
    order_grouped = block_order.reshape(groups, row_count)
    wanted = jnp.take_along_axis(targets.reshape(groups, row_count), order_grouped, axis=1)

    def make_factor(pair):
        features = feature_block(pair[0], pair[1], frequencies, phases).astype(jnp.float32)
        features = features.reshape(BLOCKS_DEV, BLOCK, FEATURES)
        gram = jnp.einsum('bid,bjd->bij', features, features, precision=highest)
        return jnp.linalg.cholesky(gram + jnp.eye(BLOCK, dtype=jnp.float32))
    factors = lax.map(make_factor, (inputs_grouped, order_grouped))
    duals = jnp.zeros((groups, row_count), jnp.float32)
    margins = jnp.zeros((groups, row_count), jnp.float32)
    weights = jnp.zeros((FEATURES,), jnp.float32)
    records = []
    for round_index in range(ROUNDS):
        residual = (wanted - duals - margins).reshape(groups, BLOCKS_DEV, BLOCK)
        update = jax.vmap(jax.vmap(solve_block))(factors, residual).reshape(groups, row_count)
        duals = duals + update
        update_bf = lax.optimization_barrier(update.astype(jnp.bfloat16))

        def contribution(triple):
            features = feature_block(triple[0], triple[1], frequencies, phases).astype(jnp.float32)
            return jnp.dot(triple[2].astype(jnp.float32), features, precision=highest) * step_scale
        weights = weights + lax.optimization_barrier(jnp.sum(lax.map(contribution, (inputs_grouped, order_grouped, update_bf)), axis=0))
        weight_bf = lax.optimization_barrier(weights.astype(jnp.bfloat16)).astype(jnp.float32)

        def margin_block(pair):
            features = feature_block(pair[0], pair[1], frequencies, phases).astype(jnp.float32)
            return jnp.dot(features, weight_bf, precision=highest)
        margins = lax.map(margin_block, (inputs_grouped, order_grouped))
        squares = jnp.sum((margins - wanted) ** 2)
        dual_sum = jnp.sum(duals * wanted - 0.5 * duals * duals)
        norm_value = jnp.sum(weights * weights)
        records.append(jnp.stack([squares / (2.0 * SAMPLES) + 0.5 * ridge * norm_value, dual_sum / SAMPLES - 0.5 * ridge * norm_value]))
    objectives = jnp.stack(records)
    restored = jax.vmap(lambda values, order_part: jnp.zeros_like(values).at[order_part].set(values))(duals, order_grouped)
    return (weights, restored.reshape(SAMPLES), objectives)
```

```python
import functools
import math

import jax
import jax.numpy as jnp
from jax import lax
from jax.experimental import pallas as pl
from jax.experimental.pallas import tpu as pltpu
from jax.sharding import Mesh
from jax.sharding import PartitionSpec as P

BLOCK = 256
ROUNDS = 4
PIECES = 4
MESH = pl.DeviceIdType.MESH
HIGHEST = lax.Precision.HIGHEST
F32 = jnp.float32
BF16 = jnp.bfloat16

SINE = (
    6.283185273782525,
    -41.341677476882325,
    81.60223116950678,
    -76.57499088229173,
    39.71091059155359,
)
TOP_EIGENVALUE = 519.0


def newton_schedule():
    rho = (TOP_EIGENVALUE - 1.0) / (TOP_EIGENVALUE + 1.0)
    scales = []
    while rho > 1e-4:
        scale = 2.0 / (2.0 - rho * rho)
        rho = rho * rho * scale / 2.0
        scales.append(scale)
    return scales


def dot(a, b, precision=None):
    return lax.dot_general(
        a, b, (((1,), (0,)), ((), ())), precision=precision, preferred_element_type=F32
    )


def dot_t(a, b):
    return lax.dot_general(a, b, (((1,), (1,)), ((), ())), preferred_element_type=F32)


def three_rows(value, rows):
    high = value.astype(BF16).astype(F32)
    middle = (value - high).astype(BF16).astype(F32)
    low = value - high - middle
    shape = (rows, value.shape[1])
    row = lax.broadcasted_iota(jnp.int32, shape, 0)
    tile = jnp.where(row == 0, high, jnp.where(row == 1, middle, jnp.where(row == 2, low, 0.0)))
    return tile.astype(BF16)


def kernel(
    sizes,
    order_s,
    inputs_ref,
    freq_ref,
    phase_ref,
    target_ref,
    order_ref,
    weights_out,
    duals_out,
    objectives_out,
    inputs_f,
    picked_f,
    picked_b,
    chosen,
    freq,
    phases,
    phi,
    gram,
    pair,
    inverse,
    rs_send,
    rs_recv,
    x_buf,
    z_buf,
    ag_buf,
    dual_buf,
    stat_f,
    stat_x,
    stat_z,
    sem_piece,
    sem_phase,
    sem_rs,
    sem_x,
    sem_z,
    sem_ag,
    sem_dual,
    sem_stat_f,
    sem_stat_x,
    sem_stat_z,
    out_right,
    out_left,
    out_relay,
    out_partner,
    out_phase,
    out_rs,
    out_x,
    out_z,
    out_ag,
    out_dual,
    out_stat_f,
    out_stat_x,
    out_stat_z,
):
    nx, nz, ny, nc = sizes
    nf = ny * nc
    rows = inputs_ref.shape[0]
    raw = inputs_ref.shape[1]
    width = freq_ref.shape[1]
    total_features = width * nf
    total_samples = rows * nx * nz
    piece = width // PIECES
    step_scale = BLOCK / total_samples
    ridge = 1.0 / BLOCK
    mx, mz = lax.axis_index("x"), lax.axis_index("z")
    my, mc = lax.axis_index("y"), lax.axis_index("core")
    me = my * nc + mc

    def feat_at(dy, dc):
        y = lax.rem(my + dy, ny)
        c = lax.rem(mc + dc, nc)
        return y, c, y * nc + c

    others = sorted(
        [(dy, dc) for dy in range(ny) for dc in range(nc) if (dy, dc) != (0, 0)],
        key=lambda o: (-min(o[0], ny - o[0]), o[1]),
    )

    barrier = pltpu.get_barrier_semaphore()
    for dy, dc in others:
        y, c, _ = feat_at(dy, dc)
        pl.semaphore_signal(barrier, inc=1, device_id={"y": y, "core": c}, device_id_type=MESH)
    for d in range(1, nx):
        pl.semaphore_signal(
            barrier, inc=1, device_id={"x": lax.rem(mx + d, nx)}, device_id_type=MESH
        )
    for d in range(1, nz):
        pl.semaphore_signal(
            barrier, inc=1, device_id={"z": lax.rem(mz + d, nz)}, device_id_type=MESH
        )

    lane = lax.broadcasted_iota(jnp.int32, (rows, 128), 1)
    inputs_f[...] = jnp.where((lane >= raw) & (lane < raw + 3), 1.0, 0.0)
    inputs_f[:, 0:raw] = inputs_ref[...].astype(F32)
    base = me * BLOCK

    def pick(i, _):
        picked_f[pl.ds(i, 1), :] = inputs_f[pl.ds(order_s[base + i], 1), :]
        return 0

    lax.fori_loop(0, BLOCK, pick, 0, unroll=8)
    picked_b[...] = picked_f[...].astype(BF16)

    pl.semaphore_wait(barrier, len(others) + nx - 1 + nz - 1)

    def send(src, dst, out_sem, in_sem, device):
        copy = pltpu.make_async_remote_copy(
            src_ref=src,
            dst_ref=dst,
            send_sem=out_sem,
            recv_sem=in_sem,
            device_id=device,
            device_id_type=MESH,
        )
        copy.start()
        return copy

    def cols(q):
        return pl.ds(pl.multiple_of(q * piece, piece), piece)

    def freq_piece(shard, q):
        return freq.at[shard, pl.ds(0, raw), cols(q)]

    y_right, _, from_right = feat_at(1, 0)
    y_left, _, from_left = feat_at(ny - 1, 0)
    partner = {"core": lax.rem(mc + 1, nc)}
    half = PIECES // 2
    started = []
    for i in range(PIECES):
        q, p = i, (i + half) % PIECES
        started.append(
            send(
                freq_ref.at[:, pl.ds(q * piece, piece)],
                freq_piece(me, q),
                out_right.at[q],
                sem_piece.at[me, q],
                {"y": y_right},
            )
        )
        started.append(
            send(
                freq_ref.at[:, pl.ds(p * piece, piece)],
                freq_piece(me, p),
                out_left.at[p],
                sem_piece.at[me, p],
                {"y": y_left},
            )
        )
        started.append(
            send(
                freq_ref.at[:, pl.ds(q * piece, piece)],
                freq_piece(me, q),
                out_partner.at[me, q],
                sem_piece.at[me, q],
                partner,
            )
        )
    for k, (dy, dc) in enumerate(reversed(others)):
        y, c, _ = feat_at(dy, dc)
        started.append(
            send(
                phase_ref,
                phases.at[me],
                out_phase.at[k],
                sem_phase.at[me],
                {"y": y, "core": c},
            )
        )
    freq[me, 0:raw, :] = freq_ref[...]
    phases[me] = phase_ref[...]

    own_order = order_ref[:, pl.ds(pl.multiple_of(base, BLOCK), BLOCK)]
    for part in range(rows // BLOCK):
        sample = lax.broadcasted_iota(jnp.int32, (BLOCK, BLOCK), 0) + part * BLOCK
        chosen[part * BLOCK : (part + 1) * BLOCK, :] = jnp.where(
            sample == own_order, 1.0, 0.0
        ).astype(BF16)
    wanted = jnp.sum(dot(three_rows(target_ref[...], 16), chosen[...]), axis=0, keepdims=True)

    def arrived(shard, q):
        pltpu.make_async_remote_copy(
            src_ref=freq_piece(shard, q),
            dst_ref=freq_piece(shard, q),
            send_sem=out_relay.at[0],
            recv_sem=sem_piece.at[shard, q],
            device_id=partner,
            device_id_type=MESH,
        ).wait_recv()

    amplitude = math.sqrt(2.0 / total_features)
    coefs = [-amplitude * v for v in SINE]
    gram[...] = jnp.zeros_like(gram)

    def make_piece(shard, q):
        freq[shard, raw:128, cols(q)] = three_rows(phases[shard, :, cols(q)], 128 - raw)
        angles = dot(picked_b[...], freq[shard, :, cols(q)])
        turns = angles * (0.5 / math.pi)
        wave = jnp.abs(turns - jnp.round(turns)) - 0.25
        square = wave * wave
        value = coefs[4]
        for c in (coefs[3], coefs[2], coefs[1], coefs[0]):
            value = value * square + c
        made = (value * wave).astype(BF16)
        phi[:, pl.ds(pl.multiple_of(shard * width + q * piece, piece), piece)] = made
        gram[...] += dot_t(made, made)

    def phases_in(dy, dc):
        _, _, shard = feat_at(dy, dc)
        pltpu.make_async_remote_copy(
            src_ref=phase_ref,
            dst_ref=phases.at[shard],
            send_sem=out_phase.at[0],
            recv_sem=sem_phase.at[shard],
            device_id=partner,
            device_id_type=MESH,
        ).wait_recv()
        return shard

    def own_step(q, _):
        make_piece(me, q)
        return 0

    lax.fori_loop(0, PIECES, own_step, 0)
    shard_p = phases_in(0, 1)

    def partner_step(q, _):
        arrived(shard_p, q)
        make_piece(shard_p, q)
        return 0

    lax.fori_loop(0, PIECES, partner_step, 0)

    def forward(shard, q):
        send(
            freq_piece(shard, q),
            freq_piece(shard, q),
            out_partner.at[shard, q],
            sem_piece.at[shard, q],
            partner,
        )

    left = phases_in(ny - 1, 0)
    left_p = phases_in(ny - 1, 1)
    right = phases_in(1, 0)
    right_p = phases_in(1, 1)
    for i in range(PIECES):
        q, p = i, (i + half) % PIECES
        arrived(left, q)
        if i < half:
            send(freq_piece(left, q), freq_piece(left, q), out_relay.at[q], sem_piece.at[left, q], {"y": y_right})
        forward(left, q)
        arrived(right, p)
        if i < half:
            send(freq_piece(right, p), freq_piece(right, p), out_relay.at[p], sem_piece.at[right, p], {"y": y_left})
        forward(right, p)
        make_piece(left, q)
        make_piece(right, p)
        arrived(left_p, q)
        make_piece(left_p, q)
        arrived(right_p, p)
        make_piece(right_p, p)
    far = phases_in(2, 0)
    far_p = phases_in(2, 1)
    for i in range(half):
        for q in (i, i + half):
            arrived(far, q)
            forward(far, q)
            make_piece(far, q)
            arrived(far_p, q)
            make_piece(far_p, q)

    row = lax.broadcasted_iota(jnp.int32, (BLOCK, BLOCK), 0)
    eye = jnp.where(row == lax.broadcasted_iota(jnp.int32, (BLOCK, BLOCK), 1), 1.0, 0.0)
    scales = newton_schedule()
    first = 2.0 / (1.0 + TOP_EIGENVALUE)
    gram[...] += eye
    error = eye - first * gram[...]
    pair[0:BLOCK, :] = (scales[0] * first) * (eye + error)
    pair[BLOCK:, :] = (1.0 - scales[0]) * eye + scales[0] * dot(error, error, HIGHEST)

    def newton(k, _):
        scale = jnp.float32(scales[1])
        for n in range(2, len(scales)):
            scale = jnp.where(k == n, jnp.float32(scales[n]), scale)
        product = dot(pair[...], pair[BLOCK:, :], HIGHEST)
        pair[0:BLOCK, :] = scale * (pair[0:BLOCK, :] + product[0:BLOCK, :])
        pair[BLOCK:, :] = (1.0 - scale) * eye + scale * product[BLOCK:, :]
        return 0

    lax.fori_loop(1, len(scales), newton, 0)
    guess = pair[0:BLOCK, :]
    residual = eye - dot(gram[...], guess, HIGHEST)
    inverse[...] = guess + dot(guess, residual, HIGHEST)

    lanes = lax.broadcasted_iota(jnp.int32, (1, 128), 1)

    def exchange(buf, sem_in, sem_out, at, mine, count, axis):
        copies = []
        for d in range(1, count):
            copies.append(
                send(
                    buf.at[at, mine],
                    buf.at[at, mine],
                    sem_out.at[d],
                    sem_in.at[at, mine],
                    {axis: lax.rem(mine + d, count)},
                )
            )
        for d in range(1, count):
            source = lax.rem(mine + d, count)
            pltpu.make_async_remote_copy(
                src_ref=buf.at[at, source],
                dst_ref=buf.at[at, source],
                send_sem=sem_out.at[d],
                recv_sem=sem_in.at[at, source],
                device_id={axis: source},
                device_id_type=MESH,
            ).wait_recv()
        return copies

    def feat_wait(buf, sem_in, sem_out, at, dy, dc):
        y, c, source = feat_at(dy, dc)
        pltpu.make_async_remote_copy(
            src_ref=buf.at[at, source],
            dst_ref=buf.at[at, source],
            send_sem=sem_out.at[0],
            recv_sem=sem_in.at[at, source],
            device_id={"y": y, "core": c},
            device_id_type=MESH,
        ).wait_recv()
        return source

    def added(buf, at, count):
        value = buf[at, 0]
        for k in range(1, count):
            value = value + buf[at, k]
        return value

    def features_of(shard):
        return phi[:, pl.ds(pl.multiple_of(shard * width, width), width)]

    def spread(value, count):
        return jnp.broadcast_to(value, (count, value.shape[1]))

    def one_round(r, carry):
        alpha, margins, weights, stats = carry
        rest = spread(wanted - alpha - margins, 8)
        delta = dot(rest, inverse[...], HIGHEST)[0:1, :]
        alpha = alpha + delta
        delta_b = spread(delta, 16).astype(BF16)
        copies = []
        for k, (dy, dc) in enumerate(others):
            y, c, target = feat_at(dy, dc)
            rs_send[r, k] = dot(delta_b, features_of(target))[0:1, :] * step_scale
            copies.append(
                send(
                    rs_send.at[r, k],
                    rs_recv.at[r, me],
                    out_rs.at[k],
                    sem_rs.at[r, me],
                    {"y": y, "core": c},
                )
            )
        rs_recv[r, me] = dot(delta_b, features_of(me))[0:1, :] * step_scale
        for dy, dc in reversed(others):
            feat_wait(rs_recv, sem_rs, out_rs, r, dy, dc)
        part = added(rs_recv, r, nf)
        if nx > 1:
            x_buf[r, mx] = part
            copies += exchange(x_buf, sem_x, out_x, r, mx, nx, "x")
            part = added(x_buf, r, nx)
        if nz > 1:
            z_buf[r, mz] = part
            copies += exchange(z_buf, sem_z, out_z, r, mz, nz, "z")
            part = added(z_buf, r, nz)
        weights = weights + part
        ag_buf[r, me] = weights.astype(BF16).astype(F32)
        for k, (dy, dc) in enumerate(others):
            y, c, _ = feat_at(dy, dc)
            copies.append(
                send(
                    ag_buf.at[r, me],
                    ag_buf.at[r, me],
                    out_ag.at[k],
                    sem_ag.at[r, me],
                    {"y": y, "core": c},
                )
            )

        def margin_of(source):
            return dot_t(spread(ag_buf[r, source], 16).astype(BF16), features_of(source))

        total = margin_of(me)
        for dy, dc in reversed(others):
            total = total + margin_of(feat_wait(ag_buf, sem_ag, out_ag, r, dy, dc))
        margins = total[0:1, :]
        off = margins - wanted
        squares = jnp.sum(off * off, axis=1, keepdims=True)
        dual = jnp.sum(alpha * wanted - 0.5 * alpha * alpha, axis=1, keepdims=True)
        norm = jnp.sum(weights * weights, axis=1, keepdims=True) * (1.0 / (nx * nz))
        stats = jnp.where(lanes == r, squares, stats)
        stats = jnp.where(lanes == r + 8, dual, stats)
        stats = jnp.where(lanes == r + 16, norm, stats)
        for copy in copies:
            copy.wait_send()
        return alpha, margins, weights, stats

    zero = jnp.zeros((1, BLOCK), F32)
    alpha, _, weights, stats = lax.fori_loop(
        0,
        ROUNDS,
        one_round,
        (zero, zero, jnp.zeros((1, width), F32), jnp.zeros((1, 128), F32)),
    )

    copies = []
    stat_f[0, me] = stats
    for k, (dy, dc) in enumerate(others):
        y, c, _ = feat_at(dy, dc)
        copies.append(
            send(
                stat_f.at[0, me],
                stat_f.at[0, me],
                out_stat_f.at[k],
                sem_stat_f.at[0, me],
                {"y": y, "core": c},
            )
        )
    dual_buf[0, me] = jnp.sum(dot_t(three_rows(alpha, 16), chosen[...]), axis=0, keepdims=True)
    for k, (dy, dc) in enumerate(others):
        y, c, _ = feat_at(dy, dc)
        copies.append(
            send(
                dual_buf.at[0, me],
                dual_buf.at[0, me],
                out_dual.at[k],
                sem_dual.at[0, me],
                {"y": y, "core": c},
            )
        )
    weights_out[...] = weights
    for dy, dc in reversed(others):
        feat_wait(stat_f, sem_stat_f, out_stat_f, 0, dy, dc)
    stats = added(stat_f, 0, nf)
    if nx > 1:
        stat_x[0, mx] = stats
        copies += exchange(stat_x, sem_stat_x, out_stat_x, 0, mx, nx, "x")
        stats = added(stat_x, 0, nx)
    for dy, dc in reversed(others):
        feat_wait(dual_buf, sem_dual, out_dual, 0, dy, dc)
    duals_out[...] = added(dual_buf, 0, nf)
    if nz > 1:
        stat_z[0, mz] = stats
        copies += exchange(stat_z, sem_stat_z, out_stat_z, 0, mz, nz, "z")
        stats = added(stat_z, 0, nz)

    wide = jnp.broadcast_to(stats, (ROUNDS, 128))
    lane = lax.broadcasted_iota(jnp.int32, (ROUNDS, 128), 1)
    line = lax.broadcasted_iota(jnp.int32, (ROUNDS, 128), 0)

    def column(first):
        return jnp.sum(jnp.where(lane == line + first, wide, 0.0), axis=1, keepdims=True)

    squares, dual, norm = column(0), column(8), column(16)
    primal = squares / (2.0 * total_samples) + 0.5 * ridge * norm
    dual = dual / total_samples - 0.5 * ridge * norm
    side = lax.broadcasted_iota(jnp.int32, (ROUNDS, 2), 1)
    objectives_out[...] = jnp.where(side == 0, primal, dual)

    for copy in started + copies:
        copy.wait_send()
    for q in range(PIECES):
        for shard in (left, right, far):
            pltpu.make_async_remote_copy(
                src_ref=freq_piece(shard, q),
                dst_ref=freq_piece(shard, q),
                send_sem=out_partner.at[shard, q],
                recv_sem=sem_piece.at[shard, q],
                device_id=partner,
                device_id_type=MESH,
            ).wait_send()
        pltpu.make_async_remote_copy(
            src_ref=freq_piece(me, q),
            dst_ref=freq_piece(me, q),
            send_sem=out_relay.at[q],
            recv_sem=sem_piece.at[me, q],
            device_id=partner,
            device_id_type=MESH,
        ).wait_send()


def on_device(sizes, inputs, frequencies, phases, targets, block_order):
    nx, nz, ny, nc = sizes
    nf = ny * nc
    rows = inputs.shape[0]
    width = frequencies.shape[1]
    vmem = pl.BlockSpec(memory_space=pltpu.VMEM)
    dma = pltpu.SemaphoreType.DMA
    scratch = [
        pltpu.VMEM((rows, 128), F32),
        pltpu.VMEM((BLOCK, 128), F32),
        pltpu.VMEM((BLOCK, 128), BF16),
        pltpu.VMEM((rows, BLOCK), BF16),
        pltpu.VMEM((nf, 128, width), BF16),
        pltpu.VMEM((nf, 1, width), F32),
        pltpu.VMEM((BLOCK, nf * width), BF16),
        pltpu.VMEM((BLOCK, BLOCK), F32),
        pltpu.VMEM((2 * BLOCK, BLOCK), F32),
        pltpu.VMEM((BLOCK, BLOCK), F32),
        pltpu.VMEM((ROUNDS, nf, 1, width), F32),
        pltpu.VMEM((ROUNDS, nf, 1, width), F32),
        pltpu.VMEM((ROUNDS, nx, 1, width), F32),
        pltpu.VMEM((ROUNDS, nz, 1, width), F32),
        pltpu.VMEM((ROUNDS, nf, 1, width), F32),
        pltpu.VMEM((1, nf, 1, rows), F32),
        pltpu.VMEM((1, nf, 1, 128), F32),
        pltpu.VMEM((1, nx, 1, 128), F32),
        pltpu.VMEM((1, nz, 1, 128), F32),
        dma((nf, PIECES)),
        dma((nf,)),
        dma((ROUNDS, nf)),
        dma((ROUNDS, nx)),
        dma((ROUNDS, nz)),
        dma((ROUNDS, nf)),
        dma((1, nf)),
        dma((1, nf)),
        dma((1, nx)),
        dma((1, nz)),
        dma((PIECES,)),
        dma((PIECES,)),
        dma((PIECES,)),
        dma((nf, PIECES)),
        dma((nf,)),
        dma((nf,)),
        dma((nx,)),
        dma((nz,)),
        dma((nf,)),
        dma((nf,)),
        dma((nf,)),
        dma((nx,)),
        dma((nz,)),
    ]
    weights, duals, objectives = pl.pallas_call(
        functools.partial(kernel, sizes),
        out_shape=(
            jax.ShapeDtypeStruct((1, width), F32),
            jax.ShapeDtypeStruct((1, rows), F32),
            jax.ShapeDtypeStruct((ROUNDS, 2), F32),
        ),
        in_specs=[pl.BlockSpec(memory_space=pltpu.SMEM)] + [vmem] * 5,
        out_specs=(vmem, vmem, vmem),
        scratch_shapes=scratch,
        compiler_params=pltpu.CompilerParams(
            collective_id=0, has_side_effects=True, vmem_limit_bytes=60 * 1024 * 1024
        ),
        name="cocoa",
    )(
        block_order,
        inputs,
        frequencies,
        phases.reshape(1, width),
        targets.reshape(1, rows),
        block_order.reshape(1, rows),
    )
    return weights.reshape(width), duals.reshape(rows), objectives


def solution(mesh):
    devices = mesh.devices
    samp, feat = mesh.shape["samp"], mesh.shape["feat"]
    nc = 2
    ny = feat // nc
    nx = 4 if samp == 32 else 1
    nz = samp // nx
    torus = Mesh(devices.reshape(nx, nz, ny, nc), ("x", "z", "y", "core"))
    samp_axes, feat_axes = ("x", "z"), ("y", "core")
    in_specs = (
        P(samp_axes, None),
        P(None, feat_axes),
        P(feat_axes),
        P(samp_axes),
        P(samp_axes),
    )
    out_specs = (P(feat_axes), P(samp_axes), P())
    return jax.shard_map(
        functools.partial(on_device, (nx, nz, ny, nc)),
        mesh=torus,
        in_specs=in_specs,
        out_specs=out_specs,
        check_vma=False,
    )
```

```python
import functools
import math

import jax
import jax.numpy as jnp
from jax import lax
from jax.experimental import pallas as pl
from jax.experimental.pallas import tpu as pltpu
from jax.sharding import Mesh
from jax.sharding import PartitionSpec as P

BLOCK = 256
ROUNDS = 4
PIECES = 4
MESH = pl.DeviceIdType.MESH
HIGHEST = lax.Precision.HIGHEST
F32 = jnp.float32
BF16 = jnp.bfloat16

SINE = (
    6.283185273782525,
    -41.341677476882325,
    81.60223116950678,
    -76.57499088229173,
    39.71091059155359,
)
TOP_EIGENVALUE = 519.0


def newton_schedule():
    rho = (TOP_EIGENVALUE - 1.0) / (TOP_EIGENVALUE + 1.0)
    scales = []
    while rho > 1e-4:
        scale = 2.0 / (2.0 - rho * rho)
        rho = rho * rho * scale / 2.0
        scales.append(scale)
    return scales


def dot(a, b, precision=None):
    return lax.dot_general(
        a, b, (((1,), (0,)), ((), ())), precision=precision, preferred_element_type=F32
    )


def dot_t(a, b):
    return lax.dot_general(a, b, (((1,), (1,)), ((), ())), preferred_element_type=F32)


def three_rows(value, rows):
    high = value.astype(BF16).astype(F32)
    middle = (value - high).astype(BF16).astype(F32)
    low = value - high - middle
    shape = (rows, value.shape[1])
    row = lax.broadcasted_iota(jnp.int32, shape, 0)
    tile = jnp.where(row == 0, high, jnp.where(row == 1, middle, jnp.where(row == 2, low, 0.0)))
    return tile.astype(BF16)


def kernel(
    sizes,
    inputs_ref,
    freq_ref,
    phase_ref,
    target_ref,
    order_ref,
    weights_out,
    duals_out,
    objectives_out,
    picked_b,
    chosen,
    freq,
    phases,
    phi,
    gram,
    gram_in,
    pair,
    inverse,
    delta_c,
    margin_c,
    rs_send,
    rs_recv,
    x_buf,
    z_buf,
    ag_buf,
    margin_buf,
    dual_buf,
    stat_y,
    stat_x,
    stat_z,
    sem_piece,
    sem_phase,
    sem_gram,
    sem_inverse,
    sem_rs,
    sem_x,
    sem_z,
    sem_ag,
    sem_margin,
    sem_dual,
    sem_stat_y,
    sem_stat_x,
    sem_stat_z,
    out_right,
    out_left,
    out_relay,
    out_phase,
    out_swap,
    out_rs,
    out_x,
    out_z,
    out_ag,
    out_margin,
    out_dual,
    out_stat_y,
    out_stat_x,
    out_stat_z,
):
    nx, nz, ny, nc = sizes
    raw, rows = inputs_ref.shape
    width = freq_ref.shape[1]
    total_features = width * ny * nc
    total_samples = rows * nx * nz
    held = nc * BLOCK
    piece = width // PIECES
    half = PIECES // 2
    step_scale = BLOCK / total_samples
    ridge = 1.0 / BLOCK
    mx, mz = lax.axis_index("x"), lax.axis_index("z")
    my, mc = lax.axis_index("y"), lax.axis_index("core")
    other = lax.rem(mc + 1, nc)
    partner = {"core": other}

    def y_at(d):
        return lax.rem(my + d, ny)

    y_far_first = sorted(range(1, ny), key=lambda d: (-min(d, ny - d), d))

    barrier = pltpu.get_barrier_semaphore()
    peers = [partner] + [{"y": y_at(d)} for d in y_far_first]
    peers += [{"x": lax.rem(mx + d, nx)} for d in range(1, nx)]
    peers += [{"z": lax.rem(mz + d, nz)} for d in range(1, nz)]
    for peer in peers:
        pl.semaphore_signal(barrier, inc=1, device_id=peer, device_id_type=MESH)

    own_order = order_ref[:, pl.ds(pl.multiple_of(my * held, held), held)]
    for part in range(rows // BLOCK):
        sample = lax.broadcasted_iota(jnp.int32, (BLOCK, held), 0) + part * BLOCK
        chosen[part * BLOCK : (part + 1) * BLOCK, :] = jnp.where(
            sample == own_order, 1.0, 0.0
        ).astype(BF16)
    line = lax.broadcasted_iota(jnp.int32, (128 - raw, held), 0)
    ones = jnp.where(line < 3, 1.0, 0.0)
    picked = jnp.concatenate([dot(inputs_ref[...], chosen[...]), ones], axis=0)
    picked_b[...] = jnp.transpose(picked).astype(BF16)

    pl.semaphore_wait(barrier, len(peers))

    def remote(src, dst, out_sem, in_sem, device):
        return pltpu.make_async_remote_copy(
            src_ref=src,
            dst_ref=dst,
            send_sem=out_sem,
            recv_sem=in_sem,
            device_id=device,
            device_id_type=MESH,
        )

    def send(*args):
        copy = remote(*args)
        copy.start()
        return copy

    def cols(q):
        return pl.ds(pl.multiple_of(q * piece, piece), piece)

    def freq_piece(shard, q):
        return freq.at[shard, pl.ds(0, raw), cols(q)]

    y_right, y_left, y_far = y_at(1), y_at(ny - 1), y_at(2)
    started = []
    for d in y_far_first:
        started.append(
            send(phase_ref, phases.at[my], out_phase.at[d], sem_phase.at[my], {"y": y_at(d)})
        )
    for i in range(PIECES):
        for q, out, y in ((i, out_right, y_right), ((i + half) % PIECES, out_left, y_left)):
            started.append(
                send(
                    freq_ref.at[:, pl.ds(q * piece, piece)],
                    freq_piece(my, q),
                    out.at[q],
                    sem_piece.at[my, q],
                    {"y": y},
                )
            )
    freq[my, 0:raw, :] = freq_ref[...]
    phases[my] = phase_ref[...]
    wanted = jnp.sum(dot(three_rows(target_ref[...], 16), chosen[...]), axis=0, keepdims=True)

    amplitude = math.sqrt(2.0 / total_features)
    coefs = [-amplitude * v for v in SINE]
    gram[...] = jnp.zeros_like(gram)

    def make_piece(shard, q):
        freq[shard, raw:128, cols(q)] = three_rows(phases[shard, :, cols(q)], 128 - raw)
        for b in range(nc):
            block = slice(b * BLOCK, (b + 1) * BLOCK)
            angles = dot(picked_b[block, :], freq[shard, :, cols(q)])
            turns = angles * (0.5 / math.pi)
            wave = jnp.abs(turns - jnp.round(turns)) - 0.25
            square = wave * wave
            value = coefs[4]
            for c in (coefs[3], coefs[2], coefs[1], coefs[0]):
                value = value * square + c
            made = (value * wave).astype(BF16)
            phi[block, pl.ds(pl.multiple_of(shard * width + q * piece, piece), piece)] = made
            gram[b] += dot_t(made, made)

    def own_step(q, _):
        make_piece(my, q)
        return 0

    lax.fori_loop(0, PIECES, own_step, 0)

    def arrived(shard, q):
        remote(
            freq_piece(shard, q),
            freq_piece(shard, q),
            out_relay.at[0],
            sem_piece.at[shard, q],
            {"y": y_left},
        ).wait_recv()

    def phases_in(shard):
        remote(
            phase_ref, phases.at[shard], out_phase.at[0], sem_phase.at[shard], {"y": y_left}
        ).wait_recv()

    def relay(shard, q, y):
        started.append(
            send(
                freq_piece(shard, q),
                freq_piece(shard, q),
                out_relay.at[q],
                sem_piece.at[shard, q],
                {"y": y},
            )
        )

    for shard in (y_left, y_right, y_far):
        phases_in(shard)
    for i in range(PIECES):
        q, p = i, (i + half) % PIECES
        arrived(y_left, q)
        if i < half:
            relay(y_left, q, y_right)
        arrived(y_right, p)
        if i < half:
            relay(y_right, p, y_left)
        make_piece(y_left, q)
        make_piece(y_right, p)
    for i in range(half):
        for q in (i, i + half):
            arrived(y_far, q)
            make_piece(y_far, q)

    swap = send(gram.at[other], gram_in, out_swap.at[0], sem_gram.at[0], partner)
    row = lax.broadcasted_iota(jnp.int32, (BLOCK, BLOCK), 0)
    eye = jnp.where(row == lax.broadcasted_iota(jnp.int32, (BLOCK, BLOCK), 1), 1.0, 0.0)
    swap.wait()
    gram_in[...] = gram[mc] + gram_in[...] + eye

    scales = newton_schedule()
    first = 2.0 / (1.0 + TOP_EIGENVALUE)
    error = eye - first * gram_in[...]
    pair[0:BLOCK, :] = (scales[0] * first) * (eye + error)
    pair[BLOCK:, :] = (1.0 - scales[0]) * eye + scales[0] * dot(error, error, HIGHEST)

    def newton(k, _):
        scale = jnp.float32(scales[1])
        for n in range(2, len(scales)):
            scale = jnp.where(k == n, jnp.float32(scales[n]), scale)
        product = dot(pair[...], pair[BLOCK:, :], HIGHEST)
        pair[0:BLOCK, :] = scale * (pair[0:BLOCK, :] + product[0:BLOCK, :])
        pair[BLOCK:, :] = (1.0 - scale) * eye + scale * product[BLOCK:, :]
        return 0

    lax.fori_loop(1, len(scales), newton, 0)
    guess = pair[0:BLOCK, :]
    residual = eye - dot(gram_in[...], guess, HIGHEST)
    inverse[mc] = guess + dot(guess, residual, HIGHEST)
    started.append(
        send(inverse.at[mc], inverse.at[mc], out_swap.at[1], sem_inverse.at[mc], partner)
    )
    remote(
        inverse.at[other], inverse.at[other], out_swap.at[1], sem_inverse.at[other], partner
    ).wait_recv()

    lanes = lax.broadcasted_iota(jnp.int32, (1, 128), 1)

    def exchange(buf, sem_in, sem_out, at, mine, count, axis):
        copies = []
        for d in range(1, count):
            copies.append(
                send(
                    buf.at[at, mine],
                    buf.at[at, mine],
                    sem_out.at[d],
                    sem_in.at[at, mine],
                    {axis: lax.rem(mine + d, count)},
                )
            )
        for d in range(1, count):
            source = lax.rem(mine + d, count)
            received(buf, sem_in, sem_out, at, source, {axis: source})
        return copies

    def received(buf, sem_in, sem_out, at, source, device):
        remote(
            buf.at[at, source],
            buf.at[at, source],
            sem_out.at[0],
            sem_in.at[at, source],
            device,
        ).wait_recv()

    def added(buf, at, count):
        value = buf[at, 0]
        for k in range(1, count):
            value = value + buf[at, k]
        return value

    group = min(512, width)

    def weigh(shard):
        done = []
        for g in range(width // group):
            at = pl.ds(pl.multiple_of(shard * width + g * group, group), group)
            total = jnp.zeros((16, group), F32)
            for t in range(held // 16):
                by = delta_c[t * 16 : (t + 1) * 16, :]
                by = jnp.concatenate([by] * (group // 128), axis=1)
                total = total + phi[t * 16 : (t + 1) * 16, at].astype(F32) * by
            done.append(jnp.sum(total, axis=0, keepdims=True))
        return jnp.concatenate(done, axis=1) * step_scale

    def add_margins(shard, weight):
        used = weight.astype(BF16).astype(F32)
        tall = 64

        def some_rows(t, _):
            at = pl.ds(pl.multiple_of(t * tall, tall), tall)
            total = margin_c[at, :]
            for g in range(width // 128):
                columns = pl.ds(pl.multiple_of(shard * width + g * 128, 128), 128)
                total = total + phi[at, columns].astype(F32) * used[:, g * 128 : (g + 1) * 128]
            margin_c[at, :] = total
            return 0

        lax.fori_loop(0, held // tall, some_rows, 0)

    def one_round(r, carry):
        alpha, margins, weights, squares_row, duals_row, norms = carry
        rest = wanted - alpha - margins
        parts = []
        for b in range(nc):
            block = inverse[b] * rest[:, b * BLOCK : (b + 1) * BLOCK]
            parts.append(jnp.sum(block, axis=1, keepdims=True))
        column = jnp.broadcast_to(jnp.concatenate(parts, axis=0), (held, 128))
        delta_c[...] = column.astype(BF16).astype(F32)
        copies = []
        for d in y_far_first:
            rs_send[r, d] = weigh(y_at(d))
            copies.append(
                send(
                    rs_send.at[r, d],
                    rs_recv.at[r, my],
                    out_rs.at[d],
                    sem_rs.at[r, my],
                    {"y": y_at(d)},
                )
            )
        rs_recv[r, my] = weigh(my)
        turned = jnp.concatenate(
            [
                jnp.transpose(column[t * 128 : (t + 1) * 128, :])[0:1, :]
                for t in range(held // 128)
            ],
            axis=1,
        )
        alpha = alpha + turned
        for d in range(1, ny):
            received(rs_recv, sem_rs, out_rs, r, y_at(d), {"y": y_at(d)})
        part = added(rs_recv, r, ny)
        if nx > 1:
            x_buf[r, mx] = part
            copies += exchange(x_buf, sem_x, out_x, r, mx, nx, "x")
            part = added(x_buf, r, nx)
        if nz > 1:
            z_buf[r, mz] = part
            copies += exchange(z_buf, sem_z, out_z, r, mz, nz, "z")
            part = added(z_buf, r, nz)
        weights = weights + part
        ag_buf[r, my] = weights
        for d in y_far_first:
            copies.append(
                send(
                    ag_buf.at[r, my],
                    ag_buf.at[r, my],
                    out_ag.at[d],
                    sem_ag.at[r, my],
                    {"y": y_at(d)},
                )
            )
        margin_c[...] = jnp.zeros_like(margin_c)
        add_margins(my, weights)
        for d in reversed(y_far_first):
            received(ag_buf, sem_ag, out_ag, r, y_at(d), {"y": y_at(d)})
            add_margins(y_at(d), ag_buf[r, y_at(d)])
        row = jnp.concatenate(
            [
                jnp.sum(
                    jnp.transpose(margin_c[t * 128 : (t + 1) * 128, :]), axis=0, keepdims=True
                )
                for t in range(held // 128)
            ],
            axis=1,
        )
        whole = ag_buf[r, 0] * ag_buf[r, 0]
        for k in range(1, ny):
            whole = whole + ag_buf[r, k] * ag_buf[r, k]
        norm = jnp.sum(whole, axis=1, keepdims=True)
        margin_buf[r, mc, :, 0:held] = row
        margin_buf[r, mc, :, held:] = jnp.broadcast_to(norm, (1, 128))
        copies.append(
            send(
                margin_buf.at[r, mc],
                margin_buf.at[r, mc],
                out_margin.at[0],
                sem_margin.at[r, mc],
                partner,
            )
        )
        received(margin_buf, sem_margin, out_margin, r, other, partner)
        both = added(margin_buf, r, nc)
        margins = both[:, 0:held]
        norms = jnp.where(lanes == r, both[:, held:], norms)
        off = margins - wanted
        squares = jnp.sum(off * off, axis=1, keepdims=True)
        dual = jnp.sum(alpha * wanted - 0.5 * alpha * alpha, axis=1, keepdims=True)
        squares_row = jnp.where(lanes == r, squares, squares_row)
        duals_row = jnp.where(lanes == r, dual, duals_row)
        for copy in copies:
            copy.wait_send()
        return alpha, margins, weights, squares_row, duals_row, norms

    zero = jnp.zeros((1, held), F32)
    blank = jnp.zeros((1, 128), F32)
    alpha, _, weights, squares_row, duals_row, norms = lax.fori_loop(
        0,
        ROUNDS,
        one_round,
        (zero, zero, jnp.zeros((1, width), F32), blank, blank, blank),
    )

    copies = []
    stat_y[0, my] = jnp.concatenate([squares_row, duals_row], axis=0)
    for d in y_far_first:
        copies.append(
            send(
                stat_y.at[0, my],
                stat_y.at[0, my],
                out_stat_y.at[d],
                sem_stat_y.at[0, my],
                {"y": y_at(d)},
            )
        )
    dual_buf[0, my] = jnp.sum(dot_t(three_rows(alpha, 16), chosen[...]), axis=0, keepdims=True)
    for d in y_far_first:
        copies.append(
            send(
                dual_buf.at[0, my],
                dual_buf.at[0, my],
                out_dual.at[d],
                sem_dual.at[0, my],
                {"y": y_at(d)},
            )
        )
    weights_out[...] = weights
    for d in range(1, ny):
        received(stat_y, sem_stat_y, out_stat_y, 0, y_at(d), {"y": y_at(d)})
    stats = added(stat_y, 0, ny)
    if nx > 1:
        stat_x[0, mx] = stats
        copies += exchange(stat_x, sem_stat_x, out_stat_x, 0, mx, nx, "x")
        stats = added(stat_x, 0, nx)
    for d in range(1, ny):
        received(dual_buf, sem_dual, out_dual, 0, y_at(d), {"y": y_at(d)})
    duals_out[...] = added(dual_buf, 0, ny)
    if nz > 1:
        stat_z[0, mz] = stats
        copies += exchange(stat_z, sem_stat_z, out_stat_z, 0, mz, nz, "z")
        stats = added(stat_z, 0, nz)
    primal = stats[0:1, :] / (2.0 * total_samples) + 0.5 * ridge * norms
    dual = stats[1:2, :] / total_samples - 0.5 * ridge * norms
    objectives_out[0:1, :] = primal[:, 0:ROUNDS]
    objectives_out[1:2, :] = dual[:, 0:ROUNDS]
    for copy in started + copies:
        copy.wait_send()


def on_device(sizes, inputs, frequencies, phases, targets, block_order):
    nx, nz, ny, nc = sizes
    rows, raw = inputs.shape
    width = frequencies.shape[1]
    held = nc * BLOCK
    vmem = pl.BlockSpec(memory_space=pltpu.VMEM)
    dma = pltpu.SemaphoreType.DMA
    scratch = [
        pltpu.VMEM((held, 128), BF16),
        pltpu.VMEM((rows, held), BF16),
        pltpu.VMEM((ny, 128, width), BF16),
        pltpu.VMEM((ny, 1, width), F32),
        pltpu.VMEM((held, ny * width), BF16),
        pltpu.VMEM((nc, BLOCK, BLOCK), F32),
        pltpu.VMEM((BLOCK, BLOCK), F32),
        pltpu.VMEM((2 * BLOCK, BLOCK), F32),
        pltpu.VMEM((nc, BLOCK, BLOCK), F32),
        pltpu.VMEM((held, 128), F32),
        pltpu.VMEM((held, 128), F32),
        pltpu.VMEM((ROUNDS, ny, 1, width), F32),
        pltpu.VMEM((ROUNDS, ny, 1, width), F32),
        pltpu.VMEM((ROUNDS, nx, 1, width), F32),
        pltpu.VMEM((ROUNDS, nz, 1, width), F32),
        pltpu.VMEM((ROUNDS, ny, 1, width), F32),
        pltpu.VMEM((ROUNDS, nc, 1, held + 128), F32),
        pltpu.VMEM((1, ny, 1, rows), F32),
        pltpu.VMEM((1, ny, 2, 128), F32),
        pltpu.VMEM((1, nx, 2, 128), F32),
        pltpu.VMEM((1, nz, 2, 128), F32),
        dma((ny, PIECES)),
        dma((ny,)),
        dma((1,)),
        dma((nc,)),
        dma((ROUNDS, ny)),
        dma((ROUNDS, nx)),
        dma((ROUNDS, nz)),
        dma((ROUNDS, ny)),
        dma((ROUNDS, nc)),
        dma((1, ny)),
        dma((1, ny)),
        dma((1, nx)),
        dma((1, nz)),
        dma((PIECES,)),
        dma((PIECES,)),
        dma((PIECES,)),
        dma((ny,)),
        dma((2,)),
        dma((ny,)),
        dma((nx,)),
        dma((nz,)),
        dma((ny,)),
        dma((1,)),
        dma((ny,)),
        dma((ny,)),
        dma((nx,)),
        dma((nz,)),
    ]
    weights, duals, objectives = pl.pallas_call(
        functools.partial(kernel, sizes),
        out_shape=(
            jax.ShapeDtypeStruct((1, width), F32),
            jax.ShapeDtypeStruct((1, rows), F32),
            jax.ShapeDtypeStruct((2, ROUNDS), F32),
        ),
        in_specs=[vmem] * 5,
        out_specs=(vmem, vmem, vmem),
        scratch_shapes=scratch,
        compiler_params=pltpu.CompilerParams(
            collective_id=0, has_side_effects=True, vmem_limit_bytes=60 * 1024 * 1024
        ),
        name="cocoa",
    )(
        inputs.T,
        frequencies,
        phases.reshape(1, width),
        targets.reshape(1, rows),
        block_order.reshape(1, rows),
    )
    return weights.reshape(width), duals.reshape(rows), objectives.T


def solution(mesh):
    devices = mesh.devices
    samp, feat = mesh.shape["samp"], mesh.shape["feat"]
    nc = 2
    ny = feat // nc
    nx = 4 if samp == 32 else 1
    nz = samp // nx
    torus = Mesh(devices.reshape(nx, nz, ny, nc), ("x", "z", "y", "core"))
    samp_axes, feat_axes = ("x", "z"), ("y", "core")
    in_specs = (
        P(samp_axes, None),
        P(None, feat_axes),
        P(feat_axes),
        P(samp_axes),
        P(samp_axes),
    )
    out_specs = (P(feat_axes), P(samp_axes), P())
    return jax.shard_map(
        functools.partial(on_device, (nx, nz, ny, nc)),
        mesh=torus,
        in_specs=in_specs,
        out_specs=out_specs,
        check_vma=False,
    )
```

```python
import functools
import math

import jax
import jax.numpy as jnp
from jax import lax
from jax.experimental import pallas as pl
from jax.experimental.pallas import tpu as pltpu
from jax.sharding import Mesh
from jax.sharding import PartitionSpec as P

BLOCK = 256
ROUNDS = 4
PIECES = 4
MESH = pl.DeviceIdType.MESH
HIGHEST = lax.Precision.HIGHEST
F32 = jnp.float32
BF16 = jnp.bfloat16

SINE = (
    6.283185273782525,
    -41.341677476882325,
    81.60223116950678,
    -76.57499088229173,
    39.71091059155359,
)
TOP_EIGENVALUE = 519.0


def newton_schedule():
    rho = (TOP_EIGENVALUE - 1.0) / (TOP_EIGENVALUE + 1.0)
    scales = []
    while rho > 1e-4:
        scale = 2.0 / (2.0 - rho * rho)
        rho = rho * rho * scale / 2.0
        scales.append(scale)
    return scales


def dot(a, b, precision=None):
    return lax.dot_general(
        a, b, (((1,), (0,)), ((), ())), precision=precision, preferred_element_type=F32
    )


def dot_t(a, b):
    return lax.dot_general(a, b, (((1,), (1,)), ((), ())), preferred_element_type=F32)


def three_rows(value, rows):
    high = value.astype(BF16).astype(F32)
    middle = (value - high).astype(BF16).astype(F32)
    low = value - high - middle
    shape = (rows, value.shape[1])
    row = lax.broadcasted_iota(jnp.int32, shape, 0)
    tile = jnp.where(row == 0, high, jnp.where(row == 1, middle, jnp.where(row == 2, low, 0.0)))
    return tile.astype(BF16)


def kernel(
    sizes,
    inputs_ref,
    freq_ref,
    phase_ref,
    target_ref,
    order_ref,
    weights_out,
    duals_out,
    objectives_out,
    picked_b,
    chosen,
    freq,
    phases,
    phi,
    gram,
    gram_in,
    pair,
    inverse,
    delta_c,
    margin_c,
    rs_send,
    rs_recv,
    z_buf,
    ag_buf,
    margin_buf,
    dual_buf,
    stat_g,
    stat_z,
    sem_piece,
    sem_phase,
    sem_gram,
    sem_inverse,
    sem_rs,
    sem_z,
    sem_ag,
    sem_margin,
    sem_dual,
    sem_stat_g,
    sem_stat_z,
    out_right,
    out_left,
    out_relay,
    out_phase,
    out_swap,
    out_rs,
    out_z,
    out_ag,
    out_margin,
    out_dual,
    out_stat_g,
    out_stat_z,
):
    nx, nz, ny, nc = sizes
    raw, rows = inputs_ref.shape
    width = freq_ref.shape[1]
    total_features = width * ny * nc
    total_samples = rows * nx * nz
    held = nc * BLOCK
    members = ny * nx
    share = width // nx
    piece = width // PIECES
    half = PIECES // 2
    step_scale = BLOCK / total_samples
    ridge = 1.0 / BLOCK
    mx, mz = lax.axis_index("x"), lax.axis_index("z")
    my, mc = lax.axis_index("y"), lax.axis_index("core")
    other = lax.rem(mc + 1, nc)
    partner = {"core": other}

    def y_at(d):
        return lax.rem(my + d, ny)

    y_far_first = sorted(range(1, ny), key=lambda d: (-min(d, ny - d), d))

    def hops(d, n):
        return min(d, n - d)

    others = sorted(
        [(dy, dx) for dy in range(ny) for dx in range(nx) if (dy, dx) != (0, 0)],
        key=lambda o: (-hops(o[0], ny) - hops(o[1], nx), o),
    )
    mine = my * nx + mx

    def member(dy, dx):
        y, x = lax.rem(my + dy, ny), lax.rem(mx + dx, nx)
        return {"y": y, "x": x}, y * nx + x

    barrier = pltpu.get_barrier_semaphore()
    peers = [partner] + [member(dy, dx)[0] for dy, dx in others]
    peers += [{"z": lax.rem(mz + d, nz)} for d in range(1, nz)]
    for peer in peers:
        pl.semaphore_signal(barrier, inc=1, device_id=peer, device_id_type=MESH)

    own_order = order_ref[:, pl.ds(pl.multiple_of(my * held, held), held)]
    for part in range(rows // BLOCK):
        sample = lax.broadcasted_iota(jnp.int32, (BLOCK, held), 0) + part * BLOCK
        chosen[part * BLOCK : (part + 1) * BLOCK, :] = jnp.where(
            sample == own_order, 1.0, 0.0
        ).astype(BF16)
    line = lax.broadcasted_iota(jnp.int32, (128 - raw, held), 0)
    ones = jnp.where(line < 3, 1.0, 0.0)
    picked = jnp.concatenate([dot(inputs_ref[...], chosen[...]), ones], axis=0)
    picked_b[...] = jnp.transpose(picked).astype(BF16)

    pl.semaphore_wait(barrier, len(peers))

    def remote(src, dst, out_sem, in_sem, device):
        return pltpu.make_async_remote_copy(
            src_ref=src,
            dst_ref=dst,
            send_sem=out_sem,
            recv_sem=in_sem,
            device_id=device,
            device_id_type=MESH,
        )

    def send(*args):
        copy = remote(*args)
        copy.start()
        return copy

    def cols(q):
        return pl.ds(pl.multiple_of(q * piece, piece), piece)

    def freq_piece(shard, q):
        return freq.at[shard, pl.ds(0, raw), cols(q)]

    y_right, y_left, y_far = y_at(1), y_at(ny - 1), y_at(2)
    started = []
    for d in y_far_first:
        started.append(
            send(phase_ref, phases.at[my], out_phase.at[d], sem_phase.at[my], {"y": y_at(d)})
        )
    for i in range(PIECES):
        for q, out, y in ((i, out_right, y_right), ((i + half) % PIECES, out_left, y_left)):
            started.append(
                send(
                    freq_ref.at[:, pl.ds(q * piece, piece)],
                    freq_piece(my, q),
                    out.at[q],
                    sem_piece.at[my, q],
                    {"y": y},
                )
            )
    freq[my, 0:raw, :] = freq_ref[...]
    phases[my] = phase_ref[...]
    wanted = jnp.sum(dot(three_rows(target_ref[...], 16), chosen[...]), axis=0, keepdims=True)

    amplitude = math.sqrt(2.0 / total_features)
    coefs = [-amplitude * v for v in SINE]
    gram[...] = jnp.zeros_like(gram)

    def make_piece(shard, q):
        freq[shard, raw:128, cols(q)] = three_rows(phases[shard, :, cols(q)], 128 - raw)
        for b in range(nc):
            block = slice(b * BLOCK, (b + 1) * BLOCK)
            angles = dot(picked_b[block, :], freq[shard, :, cols(q)])
            turns = angles * (0.5 / math.pi)
            wave = jnp.abs(turns - jnp.round(turns)) - 0.25
            square = wave * wave
            value = coefs[4]
            for c in (coefs[3], coefs[2], coefs[1], coefs[0]):
                value = value * square + c
            made = (value * wave).astype(BF16)
            phi[block, pl.ds(pl.multiple_of(shard * width + q * piece, piece), piece)] = made
            gram[b] += dot_t(made, made)

    def own_step(q, _):
        make_piece(my, q)
        return 0

    lax.fori_loop(0, PIECES, own_step, 0)

    def arrived(shard, q):
        remote(
            freq_piece(shard, q),
            freq_piece(shard, q),
            out_relay.at[0],
            sem_piece.at[shard, q],
            {"y": y_left},
        ).wait_recv()

    def phases_in(shard):
        remote(
            phase_ref, phases.at[shard], out_phase.at[0], sem_phase.at[shard], {"y": y_left}
        ).wait_recv()

    def relay(shard, q, y):
        started.append(
            send(
                freq_piece(shard, q),
                freq_piece(shard, q),
                out_relay.at[q],
                sem_piece.at[shard, q],
                {"y": y},
            )
        )

    for shard in (y_left, y_right, y_far):
        phases_in(shard)
    for i in range(PIECES):
        q, p = i, (i + half) % PIECES
        arrived(y_left, q)
        if i < half:
            relay(y_left, q, y_right)
        arrived(y_right, p)
        if i < half:
            relay(y_right, p, y_left)
        make_piece(y_left, q)
        make_piece(y_right, p)
    for i in range(half):
        for q in (i, i + half):
            arrived(y_far, q)
            make_piece(y_far, q)

    swap = send(gram.at[other], gram_in, out_swap.at[0], sem_gram.at[0], partner)
    row = lax.broadcasted_iota(jnp.int32, (BLOCK, BLOCK), 0)
    eye = jnp.where(row == lax.broadcasted_iota(jnp.int32, (BLOCK, BLOCK), 1), 1.0, 0.0)
    swap.wait()
    gram_in[...] = gram[mc] + gram_in[...] + eye

    scales = newton_schedule()
    first = 2.0 / (1.0 + TOP_EIGENVALUE)
    error = eye - first * gram_in[...]
    pair[0:BLOCK, :] = (scales[0] * first) * (eye + error)
    pair[BLOCK:, :] = (1.0 - scales[0]) * eye + scales[0] * dot(error, error, HIGHEST)

    def newton(k, _):
        scale = jnp.float32(scales[1])
        for n in range(2, len(scales)):
            scale = jnp.where(k == n, jnp.float32(scales[n]), scale)
        product = dot(pair[...], pair[BLOCK:, :], HIGHEST)
        pair[0:BLOCK, :] = scale * (pair[0:BLOCK, :] + product[0:BLOCK, :])
        pair[BLOCK:, :] = (1.0 - scale) * eye + scale * product[BLOCK:, :]
        return 0

    lax.fori_loop(1, len(scales), newton, 0)
    guess = pair[0:BLOCK, :]
    residual = eye - dot(gram_in[...], guess, HIGHEST)
    inverse[mc] = guess + dot(guess, residual, HIGHEST)
    started.append(
        send(inverse.at[mc], inverse.at[mc], out_swap.at[1], sem_inverse.at[mc], partner)
    )
    remote(
        inverse.at[other], inverse.at[other], out_swap.at[1], sem_inverse.at[other], partner
    ).wait_recv()

    lanes = lax.broadcasted_iota(jnp.int32, (1, 128), 1)

    def exchange(buf, sem_in, sem_out, at, mine, count, axis):
        copies = []
        for d in range(1, count):
            copies.append(
                send(
                    buf.at[at, mine],
                    buf.at[at, mine],
                    sem_out.at[d],
                    sem_in.at[at, mine],
                    {axis: lax.rem(mine + d, count)},
                )
            )
        for d in range(1, count):
            source = lax.rem(mine + d, count)
            received(buf, sem_in, sem_out, at, source, {axis: source})
        return copies

    def received(buf, sem_in, sem_out, at, source, device):
        remote(
            buf.at[at, source],
            buf.at[at, source],
            sem_out.at[0],
            sem_in.at[at, source],
            device,
        ).wait_recv()

    def added(buf, at, count):
        value = buf[at, 0]
        for k in range(1, count):
            value = value + buf[at, k]
        return value

    def share_at(index, g, size):
        return pl.ds(pl.multiple_of(index * share + g * size, size), size)

    group = min(512, share)

    def weigh(index):
        done = []
        for g in range(share // group):
            at = share_at(index, g, group)
            total = jnp.zeros((16, group), F32)
            for t in range(held // 16):
                by = delta_c[t * 16 : (t + 1) * 16, :]
                by = jnp.concatenate([by] * (group // 128), axis=1)
                total = total + phi[t * 16 : (t + 1) * 16, at].astype(F32) * by
            done.append(jnp.sum(total, axis=0, keepdims=True))
        return jnp.concatenate(done, axis=1) * step_scale

    def add_margins(index, weight, first=False):
        used = weight.astype(BF16).astype(F32)
        tall = 64
        for t in range(held // tall):
            at = slice(t * tall, (t + 1) * tall)
            total = jnp.zeros((tall, 128), F32) if first else margin_c[at, :]
            for g in range(share // 128):
                columns = share_at(index, g, 128)
                total = total + phi[at, columns].astype(F32) * used[:, g * 128 : (g + 1) * 128]
            margin_c[at, :] = total

    def to_members(src, dst, out_sems, sem, at):
        copies = []
        for k, (dy, dx) in enumerate(others):
            device, _ = member(dy, dx)
            copies.append(send(src.at[at, mine], dst.at[at, mine], out_sems.at[k], sem.at[at, mine], device))
        return copies

    def from_member(buf, sem_in, sem_out, at, dy, dx):
        device, index = member(dy, dx)
        received(buf, sem_in, sem_out, at, index, device)
        return index

    def one_round(r, carry):
        alpha, margins, weights, squares_row, duals_row, norms = carry
        rest = wanted - alpha - margins
        parts = []
        for b in range(nc):
            block = inverse[b] * rest[:, b * BLOCK : (b + 1) * BLOCK]
            parts.append(jnp.sum(block, axis=1, keepdims=True))
        column = jnp.broadcast_to(jnp.concatenate(parts, axis=0), (held, 128))
        delta_c[...] = column.astype(BF16).astype(F32)
        copies = []
        for k, (dy, dx) in enumerate(others):
            device, index = member(dy, dx)
            rs_send[r, k] = weigh(index)
            copies.append(
                send(rs_send.at[r, k], rs_recv.at[r, mine], out_rs.at[k], sem_rs.at[r, mine], device)
            )
        rs_recv[r, mine] = weigh(mine)
        turned = jnp.concatenate(
            [
                jnp.transpose(column[t * 128 : (t + 1) * 128, :])[0:1, :]
                for t in range(held // 128)
            ],
            axis=1,
        )
        alpha = alpha + turned
        for dy, dx in reversed(others):
            from_member(rs_recv, sem_rs, out_rs, r, dy, dx)
        part = added(rs_recv, r, members)
        if nz > 1:
            z_buf[r, mz] = part
            copies += exchange(z_buf, sem_z, out_z, r, mz, nz, "z")
            part = added(z_buf, r, nz)
        weights = weights + part
        ag_buf[r, mine] = weights
        copies += to_members(ag_buf, ag_buf, out_ag, sem_ag, r)
        add_margins(mine, weights, first=True)
        for dy, dx in reversed(others):
            index = from_member(ag_buf, sem_ag, out_ag, r, dy, dx)
            add_margins(index, ag_buf[r, index])
        row = jnp.concatenate(
            [
                jnp.sum(
                    jnp.transpose(margin_c[t * 128 : (t + 1) * 128, :]), axis=0, keepdims=True
                )
                for t in range(held // 128)
            ],
            axis=1,
        )
        whole = ag_buf[r, 0] * ag_buf[r, 0]
        for k in range(1, members):
            whole = whole + ag_buf[r, k] * ag_buf[r, k]
        norm = jnp.sum(whole, axis=1, keepdims=True)
        margin_buf[r, mc, :, 0:held] = row
        margin_buf[r, mc, :, held:] = jnp.broadcast_to(norm, (1, 128))
        copies.append(
            send(
                margin_buf.at[r, mc],
                margin_buf.at[r, mc],
                out_margin.at[0],
                sem_margin.at[r, mc],
                partner,
            )
        )
        received(margin_buf, sem_margin, out_margin, r, other, partner)
        both = added(margin_buf, r, nc)
        margins = both[:, 0:held]
        norms = jnp.where(lanes == r, both[:, held:], norms)
        off = margins - wanted
        squares = jnp.sum(off * off, axis=1, keepdims=True)
        dual = jnp.sum(alpha * wanted - 0.5 * alpha * alpha, axis=1, keepdims=True)
        squares_row = jnp.where(lanes == r, squares, squares_row)
        duals_row = jnp.where(lanes == r, dual, duals_row)
        for copy in copies:
            copy.wait_send()
        return alpha, margins, weights, squares_row, duals_row, norms

    zero = jnp.zeros((1, held), F32)
    blank = jnp.zeros((1, 128), F32)
    alpha, _, _, squares_row, duals_row, norms = lax.fori_loop(
        0,
        ROUNDS,
        one_round,
        (zero, zero, jnp.zeros((1, share), F32), blank, blank, blank),
    )

    stat_g[0, mine] = jnp.concatenate([squares_row, duals_row], axis=0)
    copies = to_members(stat_g, stat_g, out_stat_g, sem_stat_g, 0)
    dual_buf[0, my] = jnp.sum(dot_t(three_rows(alpha, 16), chosen[...]), axis=0, keepdims=True)
    for d in y_far_first:
        copies.append(
            send(
                dual_buf.at[0, my],
                dual_buf.at[0, my],
                out_dual.at[d],
                sem_dual.at[0, my],
                {"y": y_at(d)},
            )
        )
    weights_out[...] = jnp.concatenate(
        [ag_buf[ROUNDS - 1, my * nx + k] for k in range(nx)], axis=1
    )
    for dy, dx in reversed(others):
        from_member(stat_g, sem_stat_g, out_stat_g, 0, dy, dx)
    stats = added(stat_g, 0, members)
    if nz > 1:
        stat_z[0, mz] = stats
        copies += exchange(stat_z, sem_stat_z, out_stat_z, 0, mz, nz, "z")
        stats = added(stat_z, 0, nz)
    for d in range(1, ny):
        received(dual_buf, sem_dual, out_dual, 0, y_at(d), {"y": y_at(d)})
    duals_out[...] = added(dual_buf, 0, ny)
    primal = stats[0:1, :] / (2.0 * total_samples) + 0.5 * ridge * norms
    dual = stats[1:2, :] / total_samples - 0.5 * ridge * norms
    objectives_out[0:1, :] = primal[:, 0:ROUNDS]
    objectives_out[1:2, :] = dual[:, 0:ROUNDS]
    for copy in started + copies:
        copy.wait_send()


def on_device(sizes, inputs, frequencies, phases, targets, block_order):
    nx, nz, ny, nc = sizes
    rows, raw = inputs.shape
    width = frequencies.shape[1]
    held = nc * BLOCK
    members = ny * nx
    share = width // nx
    vmem = pl.BlockSpec(memory_space=pltpu.VMEM)
    dma = pltpu.SemaphoreType.DMA
    scratch = [
        pltpu.VMEM((held, 128), BF16),
        pltpu.VMEM((rows, held), BF16),
        pltpu.VMEM((ny, 128, width), BF16),
        pltpu.VMEM((ny, 1, width), F32),
        pltpu.VMEM((held, ny * width), BF16),
        pltpu.VMEM((nc, BLOCK, BLOCK), F32),
        pltpu.VMEM((BLOCK, BLOCK), F32),
        pltpu.VMEM((2 * BLOCK, BLOCK), F32),
        pltpu.VMEM((nc, BLOCK, BLOCK), F32),
        pltpu.VMEM((held, 128), F32),
        pltpu.VMEM((held, 128), F32),
        pltpu.VMEM((ROUNDS, members, 1, share), F32),
        pltpu.VMEM((ROUNDS, members, 1, share), F32),
        pltpu.VMEM((ROUNDS, nz, 1, share), F32),
        pltpu.VMEM((ROUNDS, members, 1, share), F32),
        pltpu.VMEM((ROUNDS, nc, 1, held + 128), F32),
        pltpu.VMEM((1, ny, 1, rows), F32),
        pltpu.VMEM((1, members, 2, 128), F32),
        pltpu.VMEM((1, nz, 2, 128), F32),
        dma((ny, PIECES)),
        dma((ny,)),
        dma((1,)),
        dma((nc,)),
        dma((ROUNDS, members)),
        dma((ROUNDS, nz)),
        dma((ROUNDS, members)),
        dma((ROUNDS, nc)),
        dma((1, ny)),
        dma((1, members)),
        dma((1, nz)),
        dma((PIECES,)),
        dma((PIECES,)),
        dma((PIECES,)),
        dma((ny,)),
        dma((2,)),
        dma((members,)),
        dma((nz,)),
        dma((members,)),
        dma((1,)),
        dma((ny,)),
        dma((members,)),
        dma((nz,)),
    ]
    weights, duals, objectives = pl.pallas_call(
        functools.partial(kernel, sizes),
        out_shape=(
            jax.ShapeDtypeStruct((1, width), F32),
            jax.ShapeDtypeStruct((1, rows), F32),
            jax.ShapeDtypeStruct((2, ROUNDS), F32),
        ),
        in_specs=[vmem] * 5,
        out_specs=(vmem, vmem, vmem),
        scratch_shapes=scratch,
        compiler_params=pltpu.CompilerParams(
            collective_id=0, has_side_effects=True, vmem_limit_bytes=60 * 1024 * 1024
        ),
        name="cocoa",
    )(
        inputs.T,
        frequencies,
        phases.reshape(1, width),
        targets.reshape(1, rows),
        block_order.reshape(1, rows),
    )
    return weights.reshape(width), duals.reshape(rows), objectives.T


def solution(mesh):
    devices = mesh.devices
    samp, feat = mesh.shape["samp"], mesh.shape["feat"]
    nc = 2
    ny = feat // nc
    nx = math.gcd(samp, 4)
    nz = samp // nx
    torus = Mesh(devices.reshape(nx, nz, ny, nc), ("x", "z", "y", "core"))
    samp_axes, feat_axes = ("x", "z"), ("y", "core")
    in_specs = (
        P(samp_axes, None),
        P(None, feat_axes),
        P(feat_axes),
        P(samp_axes),
        P(samp_axes),
    )
    out_specs = (P(feat_axes), P(samp_axes), P())
    return jax.shard_map(
        functools.partial(on_device, (nx, nz, ny, nc)),
        mesh=torus,
        in_specs=in_specs,
        out_specs=out_specs,
        check_vma=False,
    )
```

```python
import functools
import math

import jax
import jax.numpy as jnp
from jax import lax
from jax.experimental import pallas as pl
from jax.experimental.pallas import tpu as pltpu
from jax.sharding import Mesh
from jax.sharding import PartitionSpec as P

BLOCK = 256
ROUNDS = 4
PIECES = 4
MESH = pl.DeviceIdType.MESH
HIGHEST = lax.Precision.HIGHEST
F32 = jnp.float32
BF16 = jnp.bfloat16

SINE = (
    6.283185273782525,
    -41.341677476882325,
    81.60223116950678,
    -76.57499088229173,
    39.71091059155359,
)
TOP_EIGENVALUE = 519.0


def newton_schedule():
    rho = (TOP_EIGENVALUE - 1.0) / (TOP_EIGENVALUE + 1.0)
    scales = []
    while rho > 1e-4:
        scale = 2.0 / (2.0 - rho * rho)
        rho = rho * rho * scale / 2.0
        scales.append(scale)
    return scales


def dot(a, b, precision=None):
    return lax.dot_general(
        a, b, (((1,), (0,)), ((), ())), precision=precision, preferred_element_type=F32
    )


def dot_t(a, b):
    return lax.dot_general(a, b, (((1,), (1,)), ((), ())), preferred_element_type=F32)


def three_rows(value, rows):
    high = value.astype(BF16).astype(F32)
    middle = (value - high).astype(BF16).astype(F32)
    low = value - high - middle
    shape = (rows, value.shape[1])
    row = lax.broadcasted_iota(jnp.int32, shape, 0)
    tile = jnp.where(row == 0, high, jnp.where(row == 1, middle, jnp.where(row == 2, low, 0.0)))
    return tile.astype(BF16)


def kernel(
    sizes,
    inputs_hbm,
    freq_hbm,
    phase_hbm,
    target_hbm,
    order_hbm,
    weights_out,
    duals_out,
    objectives_out,
    inputs_ref,
    target_ref,
    order_ref,
    picked_b,
    chosen,
    freq,
    phases,
    phi,
    gram,
    gram_in,
    pair,
    inverse,
    delta_c,
    margin_c,
    margin_rows,
    alpha_rows,
    rs_send,
    rs_recv,
    z_buf,
    ag_buf,
    margin_buf,
    norm_buf,
    dual_buf,
    stat_g,
    stat_z,
    sem_in,
    sem_piece,
    sem_phase,
    sem_gram,
    sem_inverse,
    sem_rs,
    sem_z,
    sem_ag,
    sem_margin,
    sem_norm,
    sem_dual,
    sem_stat_g,
    sem_stat_z,
    out_right,
    out_left,
    out_relay,
    out_phase,
    out_swap,
    out_rs,
    out_z,
    out_ag,
    out_margin,
    out_dual,
    out_stat_g,
    out_stat_z,
):
    nx, nz, ny, nc = sizes
    raw, rows = inputs_hbm.shape
    width = freq_hbm.shape[1]
    total_features = width * ny * nc
    total_samples = rows * nx * nz
    held = nc * BLOCK
    members = ny * nx
    share = width // nx
    piece = width // PIECES
    half = PIECES // 2
    step_scale = BLOCK / total_samples
    ridge = 1.0 / BLOCK
    mx, mz = lax.axis_index("x"), lax.axis_index("z")
    my, mc = lax.axis_index("y"), lax.axis_index("core")
    other = lax.rem(mc + 1, nc)
    partner = {"core": other}

    def y_at(d):
        return lax.rem(my + d, ny)

    y_far_first = sorted(range(1, ny), key=lambda d: (-min(d, ny - d), d))

    def hops(d, n):
        return min(d, n - d)

    others = sorted(
        [(dy, dx) for dy in range(ny) for dx in range(nx) if (dy, dx) != (0, 0)],
        key=lambda o: (-hops(o[0], ny) - hops(o[1], nx), o),
    )
    mine = my * nx + mx

    def member(dy, dx):
        y, x = lax.rem(my + dy, ny), lax.rem(mx + dx, nx)
        return {"y": y, "x": x}, y * nx + x

    barrier = pltpu.get_barrier_semaphore()
    peers = [partner] + [member(dy, dx)[0] for dy, dx in others]
    peers += [{"z": lax.rem(mz + d, nz)} for d in range(1, nz)]
    for peer in peers:
        pl.semaphore_signal(barrier, inc=1, device_id=peer, device_id_type=MESH)
    loads = [
        pltpu.make_async_copy(src, dst, sem_in.at[k])
        for k, (src, dst) in enumerate(
            [
                (order_hbm, order_ref),
                (inputs_hbm, inputs_ref),
                (freq_hbm, freq.at[my, pl.ds(0, raw), :]),
                (phase_hbm, phases.at[my]),
                (target_hbm, target_ref),
            ]
        )
    ]
    for load in loads:
        load.start()
    loads[0].wait()

    own_order = order_ref[:, pl.ds(pl.multiple_of(my * held, held), held)]
    for part in range(rows // BLOCK):
        sample = lax.broadcasted_iota(jnp.int32, (BLOCK, held), 0) + part * BLOCK
        chosen[part * BLOCK : (part + 1) * BLOCK, :] = jnp.where(
            sample == own_order, 1.0, 0.0
        ).astype(BF16)
    line = lax.broadcasted_iota(jnp.int32, (128 - raw, held), 0)
    ones = jnp.where(line < 3, 1.0, 0.0)
    loads[1].wait()
    picked = jnp.concatenate([dot(inputs_ref[...], chosen[...]), ones], axis=0)
    picked_b[...] = jnp.transpose(picked).astype(BF16)

    for load in loads[2:]:
        load.wait()
    pl.semaphore_wait(barrier, len(peers))

    def remote(src, dst, out_sem, in_sem, device):
        return pltpu.make_async_remote_copy(
            src_ref=src,
            dst_ref=dst,
            send_sem=out_sem,
            recv_sem=in_sem,
            device_id=device,
            device_id_type=MESH,
        )

    def send(*args):
        copy = remote(*args)
        copy.start()
        return copy

    def cols(q):
        return pl.ds(pl.multiple_of(q * piece, piece), piece)

    def freq_piece(shard, q):
        return freq.at[shard, pl.ds(0, raw), cols(q)]

    y_right, y_left, y_far = y_at(1), y_at(ny - 1), y_at(2)
    started = []
    for d in y_far_first:
        started.append(
            send(phases.at[my], phases.at[my], out_phase.at[d], sem_phase.at[my], {"y": y_at(d)})
        )
    for i in range(PIECES):
        for q, out, y in ((i, out_right, y_right), ((i + half) % PIECES, out_left, y_left)):
            started.append(
                send(
                    freq_piece(my, q),
                    freq_piece(my, q),
                    out.at[q],
                    sem_piece.at[my, q],
                    {"y": y},
                )
            )
    wanted = jnp.sum(dot(three_rows(target_ref[...], 16), chosen[...]), axis=0, keepdims=True)

    amplitude = math.sqrt(2.0 / total_features)
    coefs = [-amplitude * v for v in SINE]
    gram[...] = jnp.zeros_like(gram)

    def make_piece(shard, q):
        freq[shard, raw:128, cols(q)] = three_rows(phases[shard, :, cols(q)], 128 - raw)
        for b in range(nc):
            block = slice(b * BLOCK, (b + 1) * BLOCK)
            angles = dot(picked_b[block, :], freq[shard, :, cols(q)])
            turns = angles * (0.5 / math.pi)
            wave = jnp.abs(turns - jnp.round(turns)) - 0.25
            square = wave * wave
            value = coefs[4]
            for c in (coefs[3], coefs[2], coefs[1], coefs[0]):
                value = value * square + c
            made = (value * wave).astype(BF16)
            phi[block, pl.ds(pl.multiple_of(shard * width + q * piece, piece), piece)] = made
            gram[b] += dot_t(made, made)

    def own_step(q, _):
        make_piece(my, q)
        return 0

    lax.fori_loop(0, PIECES, own_step, 0)

    def arrived(shard, q):
        remote(
            freq_piece(shard, q),
            freq_piece(shard, q),
            out_relay.at[0],
            sem_piece.at[shard, q],
            {"y": y_left},
        ).wait_recv()

    def phases_in(shard):
        remote(
            phases.at[shard], phases.at[shard], out_phase.at[0], sem_phase.at[shard], {"y": y_left}
        ).wait_recv()

    def relay(shard, q, y):
        started.append(
            send(
                freq_piece(shard, q),
                freq_piece(shard, q),
                out_relay.at[q],
                sem_piece.at[shard, q],
                {"y": y},
            )
        )

    for shard in (y_left, y_right, y_far):
        phases_in(shard)
    for i in range(PIECES):
        q, p = i, (i + half) % PIECES
        arrived(y_left, q)
        if i < half:
            relay(y_left, q, y_right)
        arrived(y_right, p)
        if i < half:
            relay(y_right, p, y_left)
        make_piece(y_left, q)
        make_piece(y_right, p)
    for i in range(half):
        for q in (i, i + half):
            arrived(y_far, q)
            make_piece(y_far, q)

    swap = send(gram.at[other], gram_in, out_swap.at[0], sem_gram.at[0], partner)
    row = lax.broadcasted_iota(jnp.int32, (BLOCK, BLOCK), 0)
    eye = jnp.where(row == lax.broadcasted_iota(jnp.int32, (BLOCK, BLOCK), 1), 1.0, 0.0)
    swap.wait()
    gram_in[...] = gram[mc] + gram_in[...] + eye

    scales = newton_schedule()
    first = 2.0 / (1.0 + TOP_EIGENVALUE)
    error = eye - first * gram_in[...]
    pair[0:BLOCK, :] = (scales[0] * first) * (eye + error)
    pair[BLOCK:, :] = (1.0 - scales[0]) * eye + scales[0] * dot(error, error, HIGHEST)

    def newton(k, _):
        scale = jnp.float32(scales[1])
        for n in range(2, len(scales)):
            scale = jnp.where(k == n, jnp.float32(scales[n]), scale)
        product = dot(pair[...], pair[BLOCK:, :], HIGHEST)
        pair[0:BLOCK, :] = scale * (pair[0:BLOCK, :] + product[0:BLOCK, :])
        pair[BLOCK:, :] = (1.0 - scale) * eye + scale * product[BLOCK:, :]
        return 0

    lax.fori_loop(1, len(scales), newton, 0)
    guess = pair[0:BLOCK, :]
    residual = eye - dot(gram_in[...], guess, HIGHEST)
    inverse[mc] = guess + dot(guess, residual, HIGHEST)
    started.append(
        send(inverse.at[mc], inverse.at[mc], out_swap.at[1], sem_inverse.at[mc], partner)
    )
    remote(
        inverse.at[other], inverse.at[other], out_swap.at[1], sem_inverse.at[other], partner
    ).wait_recv()

    lanes = lax.broadcasted_iota(jnp.int32, (1, 128), 1)

    def exchange(buf, sem_in, sem_out, at, mine, count, axis):
        copies = []
        for d in range(1, count):
            copies.append(
                send(
                    buf.at[at, mine],
                    buf.at[at, mine],
                    sem_out.at[d],
                    sem_in.at[at, mine],
                    {axis: lax.rem(mine + d, count)},
                )
            )
        for d in range(1, count):
            source = lax.rem(mine + d, count)
            received(buf, sem_in, sem_out, at, source, {axis: source})
        return copies

    def received(buf, sem_in, sem_out, at, source, device):
        remote(
            buf.at[at, source],
            buf.at[at, source],
            sem_out.at[0],
            sem_in.at[at, source],
            device,
        ).wait_recv()

    def added(buf, at, count):
        value = buf[at, 0]
        for k in range(1, count):
            value = value + buf[at, k]
        return value

    def share_at(index, g, size):
        return pl.ds(pl.multiple_of(index * share + g * size, size), size)

    group = min(512, share)

    def weigh(index):
        done = []
        for g in range(share // group):
            at = share_at(index, g, group)
            total = jnp.zeros((16, group), F32)
            for t in range(held // 16):
                by = delta_c[t * 16 : (t + 1) * 16, :]
                by = jnp.concatenate([by] * (group // 128), axis=1)
                total = total + phi[t * 16 : (t + 1) * 16, at].astype(F32) * by
            done.append(jnp.sum(total, axis=0, keepdims=True))
        return jnp.concatenate(done, axis=1) * step_scale

    def add_margins(index, weight, first=False):
        used = weight.astype(BF16).astype(F32)
        tall = 64
        for t in range(held // tall):
            at = slice(t * tall, (t + 1) * tall)
            total = jnp.zeros((tall, 128), F32) if first else margin_c[at, :]
            for g in range(share // 128):
                columns = share_at(index, g, 128)
                total = total + phi[at, columns].astype(F32) * used[:, g * 128 : (g + 1) * 128]
            margin_c[at, :] = total

    def to_members(src, dst, out_sems, sem, at):
        copies = []
        for k, (dy, dx) in enumerate(others):
            device, _ = member(dy, dx)
            copies.append(send(src.at[at, mine], dst.at[at, mine], out_sems.at[k], sem.at[at, mine], device))
        return copies

    def from_member(buf, sem_in, sem_out, at, dy, dx):
        device, index = member(dy, dx)
        received(buf, sem_in, sem_out, at, index, device)
        return index

    def one_round(r, carry):
        alpha, margins, weights = carry
        rest = wanted - alpha - margins
        parts = []
        for b in range(nc):
            block = inverse[b] * rest[:, b * BLOCK : (b + 1) * BLOCK]
            parts.append(jnp.sum(block, axis=1, keepdims=True))
        column = jnp.broadcast_to(jnp.concatenate(parts, axis=0), (held, 128))
        delta_c[...] = column.astype(BF16).astype(F32)
        copies = []
        for k, (dy, dx) in enumerate(others):
            device, index = member(dy, dx)
            rs_send[r, k] = weigh(index)
            copies.append(
                send(rs_send.at[r, k], rs_recv.at[r, mine], out_rs.at[k], sem_rs.at[r, mine], device)
            )
        rs_recv[r, mine] = weigh(mine)
        turned = jnp.concatenate(
            [
                jnp.transpose(column[t * 128 : (t + 1) * 128, :])[0:1, :]
                for t in range(held // 128)
            ],
            axis=1,
        )
        alpha = alpha + turned
        for dy, dx in reversed(others):
            from_member(rs_recv, sem_rs, out_rs, r, dy, dx)
        part = added(rs_recv, r, members)
        if nz > 1:
            z_buf[r, mz] = part
            copies += exchange(z_buf, sem_z, out_z, r, mz, nz, "z")
            part = added(z_buf, r, nz)
        weights = weights + part
        ag_buf[r, mine] = weights
        copies += to_members(ag_buf, ag_buf, out_ag, sem_ag, r)
        add_margins(mine, weights, first=True)
        for dy, dx in reversed(others):
            index = from_member(ag_buf, sem_ag, out_ag, r, dy, dx)
            add_margins(index, ag_buf[r, index])
        row = jnp.concatenate(
            [
                jnp.sum(
                    jnp.transpose(margin_c[t * 128 : (t + 1) * 128, :]), axis=0, keepdims=True
                )
                for t in range(held // 128)
            ],
            axis=1,
        )
        margin_buf[r, mc] = row
        copies.append(
            send(
                margin_buf.at[r, mc],
                margin_buf.at[r, mc],
                out_margin.at[0],
                sem_margin.at[r, mc],
                partner,
            )
        )
        received(margin_buf, sem_margin, out_margin, r, other, partner)
        margins = added(margin_buf, r, nc)
        margin_rows[r] = margins
        alpha_rows[r] = alpha
        for copy in copies:
            copy.wait_send()
        return alpha, margins, weights

    zero = jnp.zeros((1, held), F32)
    alpha, _, _ = lax.fori_loop(
        0,
        ROUNDS,
        one_round,
        (zero, zero, jnp.zeros((1, share), F32)),
    )

    def in_lanes(values):
        line = jnp.zeros((1, 128), F32)
        for r, value in enumerate(values):
            line = jnp.where(lanes == r, jnp.sum(value, axis=1, keepdims=True), line)
        return line

    squares = in_lanes([(margin_rows[r] - wanted) ** 2 for r in range(ROUNDS)])
    gains = in_lanes(
        [alpha_rows[r] * wanted - 0.5 * alpha_rows[r] * alpha_rows[r] for r in range(ROUNDS)]
    )
    stat_g[0, mine] = jnp.concatenate([squares, gains], axis=0)
    copies = to_members(stat_g, stat_g, out_stat_g, sem_stat_g, 0)
    wholes = []
    for r in range(ROUNDS):
        whole = ag_buf[r, 0] * ag_buf[r, 0]
        for k in range(1, members):
            whole = whole + ag_buf[r, k] * ag_buf[r, k]
        wholes.append(whole)
    norm_buf[0, mc] = in_lanes(wholes)
    copies.append(
        send(norm_buf.at[0, mc], norm_buf.at[0, mc], out_swap.at[2], sem_norm.at[0, mc], partner)
    )
    dual_buf[0, my] = jnp.sum(dot_t(three_rows(alpha, 16), chosen[...]), axis=0, keepdims=True)
    for d in y_far_first:
        copies.append(
            send(
                dual_buf.at[0, my],
                dual_buf.at[0, my],
                out_dual.at[d],
                sem_dual.at[0, my],
                {"y": y_at(d)},
            )
        )
    weights_out[...] = jnp.concatenate(
        [ag_buf[ROUNDS - 1, my * nx + k] for k in range(nx)], axis=1
    )
    for dy, dx in reversed(others):
        from_member(stat_g, sem_stat_g, out_stat_g, 0, dy, dx)
    stats = added(stat_g, 0, members)
    if nz > 1:
        stat_z[0, mz] = stats
        copies += exchange(stat_z, sem_stat_z, out_stat_z, 0, mz, nz, "z")
        stats = added(stat_z, 0, nz)
    for d in range(1, ny):
        received(dual_buf, sem_dual, out_dual, 0, y_at(d), {"y": y_at(d)})
    duals_out[...] = added(dual_buf, 0, ny)
    received(norm_buf, sem_norm, out_swap, 0, other, partner)
    norms = added(norm_buf, 0, nc)
    primal = stats[0:1, :] / (2.0 * total_samples) + 0.5 * ridge * norms
    dual = stats[1:2, :] / total_samples - 0.5 * ridge * norms
    objectives_out[0:1, :] = primal[:, 0:ROUNDS]
    objectives_out[1:2, :] = dual[:, 0:ROUNDS]
    for copy in started + copies:
        copy.wait_send()


def copied(weights, duals, objectives, weights_out, duals_out, objectives_out):
    weights_out[...] = weights[...]
    duals_out[...] = duals[...]
    objectives_out[...] = objectives[...]


def on_device(sizes, inputs, frequencies, phases, targets, block_order):
    nx, nz, ny, nc = sizes
    rows, raw = inputs.shape
    width = frequencies.shape[1]
    held = nc * BLOCK
    members = ny * nx
    share = width // nx
    vmem = pl.BlockSpec(memory_space=pltpu.VMEM)
    dma = pltpu.SemaphoreType.DMA
    scratch = [
        pltpu.VMEM((raw, rows), BF16),
        pltpu.VMEM((1, rows), F32),
        pltpu.VMEM((1, rows), jnp.int32),
        pltpu.VMEM((held, 128), BF16),
        pltpu.VMEM((rows, held), BF16),
        pltpu.VMEM((ny, 128, width), BF16),
        pltpu.VMEM((ny, 1, width), F32),
        pltpu.VMEM((held, ny * width), BF16),
        pltpu.VMEM((nc, BLOCK, BLOCK), F32),
        pltpu.VMEM((BLOCK, BLOCK), F32),
        pltpu.VMEM((2 * BLOCK, BLOCK), F32),
        pltpu.VMEM((nc, BLOCK, BLOCK), F32),
        pltpu.VMEM((held, 128), F32),
        pltpu.VMEM((held, 128), F32),
        pltpu.VMEM((ROUNDS, 1, held), F32),
        pltpu.VMEM((ROUNDS, 1, held), F32),
        pltpu.VMEM((ROUNDS, members, 1, share), F32),
        pltpu.VMEM((ROUNDS, members, 1, share), F32),
        pltpu.VMEM((ROUNDS, nz, 1, share), F32),
        pltpu.VMEM((ROUNDS, members, 1, share), F32),
        pltpu.VMEM((ROUNDS, nc, 1, held), F32),
        pltpu.VMEM((1, nc, 1, 128), F32),
        pltpu.VMEM((1, ny, 1, rows), F32),
        pltpu.VMEM((1, members, 2, 128), F32),
        pltpu.VMEM((1, nz, 2, 128), F32),
        dma((5,)),
        dma((ny, PIECES)),
        dma((ny,)),
        dma((1,)),
        dma((nc,)),
        dma((ROUNDS, members)),
        dma((ROUNDS, nz)),
        dma((ROUNDS, members)),
        dma((ROUNDS, nc)),
        dma((1, nc)),
        dma((1, ny)),
        dma((1, members)),
        dma((1, nz)),
        dma((PIECES,)),
        dma((PIECES,)),
        dma((PIECES,)),
        dma((ny,)),
        dma((3,)),
        dma((members,)),
        dma((nz,)),
        dma((members,)),
        dma((1,)),
        dma((ny,)),
        dma((members,)),
        dma((nz,)),
    ]
    shapes = (
        jax.ShapeDtypeStruct((1, width), F32),
        jax.ShapeDtypeStruct((1, rows), F32),
        jax.ShapeDtypeStruct((2, ROUNDS), F32),
    )
    results = pl.pallas_call(
        functools.partial(kernel, sizes),
        out_shape=shapes,
        in_specs=[pl.BlockSpec(memory_space=pl.ANY)] * 5,
        out_specs=(vmem, vmem, vmem),
        scratch_shapes=scratch,
        compiler_params=pltpu.CompilerParams(
            collective_id=0, has_side_effects=True, vmem_limit_bytes=60 * 1024 * 1024
        ),
        name="cocoa",
    )(
        inputs.T,
        frequencies,
        phases.reshape(1, width),
        targets.reshape(1, rows),
        block_order.reshape(1, rows),
    )
    weights, duals, objectives = pl.pallas_call(
        copied,
        out_shape=shapes,
        in_specs=[vmem] * 3,
        out_specs=(vmem, vmem, vmem),
        name="results",
    )(*results)
    return weights.reshape(width), duals.reshape(rows), objectives.T


def solution(mesh):
    devices = mesh.devices
    samp, feat = mesh.shape["samp"], mesh.shape["feat"]
    nc = 2
    ny = feat // nc
    nx = math.gcd(samp, 4)
    nz = samp // nx
    torus = Mesh(devices.reshape(nx, nz, ny, nc), ("x", "z", "y", "core"))
    samp_axes, feat_axes = ("x", "z"), ("y", "core")
    in_specs = (
        P(samp_axes, None),
        P(None, feat_axes),
        P(feat_axes),
        P(samp_axes),
        P(samp_axes),
    )
    out_specs = (P(feat_axes), P(samp_axes), P())
    return jax.shard_map(
        functools.partial(on_device, (nx, nz, ny, nc)),
        mesh=torus,
        in_specs=in_specs,
        out_specs=out_specs,
        check_vma=False,
    )
```

```python
import functools
import math

import jax
import jax.numpy as jnp
from jax import lax
from jax.experimental import pallas as pl
from jax.experimental.pallas import tpu as pltpu
from jax.sharding import Mesh
from jax.sharding import PartitionSpec as P

BLOCK = 256
ROUNDS = 4
PIECES = 4
MESH = pl.DeviceIdType.MESH
HIGHEST = lax.Precision.HIGHEST
F32 = jnp.float32
BF16 = jnp.bfloat16

SINE = (
    6.283185273782525,
    -41.341677476882325,
    81.60223116950678,
    -76.57499088229173,
    39.71091059155359,
)
TOP_EIGENVALUE = 519.0


def newton_schedule():
    rho = (TOP_EIGENVALUE - 1.0) / (TOP_EIGENVALUE + 1.0)
    scales = []
    while rho > 1e-4:
        scale = 2.0 / (2.0 - rho * rho)
        rho = rho * rho * scale / 2.0
        scales.append(scale)
    return scales


def dot(a, b, precision=None):
    return lax.dot_general(
        a, b, (((1,), (0,)), ((), ())), precision=precision, preferred_element_type=F32
    )


def halves(value):
    high = value.astype(BF16)
    return high, (value - high.astype(F32)).astype(BF16)


def dot_3(a, b):
    a_high, a_low = halves(a)
    b_high, b_low = halves(b)
    return dot(a_high, b_high) + (dot(a_high, b_low) + dot(a_low, b_high))


def dot_t(a, b):
    return lax.dot_general(a, b, (((1,), (1,)), ((), ())), preferred_element_type=F32)


def three_rows(value, rows):
    high = value.astype(BF16).astype(F32)
    middle = (value - high).astype(BF16).astype(F32)
    low = value - high - middle
    shape = (rows, value.shape[1])
    row = lax.broadcasted_iota(jnp.int32, shape, 0)
    tile = jnp.where(row == 0, high, jnp.where(row == 1, middle, jnp.where(row == 2, low, 0.0)))
    return tile.astype(BF16)


def kernel(
    sizes,
    inputs_hbm,
    freq_hbm,
    phase_hbm,
    target_hbm,
    order_hbm,
    weights_out,
    duals_out,
    objectives_out,
    inputs_ref,
    target_ref,
    order_ref,
    picked_b,
    chosen,
    freq,
    phases,
    phi,
    gram,
    gram_in,
    pair,
    inverse,
    delta_c,
    margin_c,
    margin_rows,
    alpha_rows,
    rs_send,
    rs_recv,
    z_buf,
    ag_buf,
    margin_buf,
    norm_buf,
    dual_buf,
    stat_g,
    stat_z,
    sem_in,
    sem_piece,
    sem_phase,
    sem_gram,
    sem_inverse,
    sem_rs,
    sem_z,
    sem_ag,
    sem_margin,
    sem_norm,
    sem_dual,
    sem_stat_g,
    sem_stat_z,
    out_right,
    out_left,
    out_relay,
    out_phase,
    out_swap,
    out_rs,
    out_z,
    out_ag,
    out_margin,
    out_dual,
    out_stat_g,
    out_stat_z,
):
    nx, nz, ny, nc = sizes
    raw, rows = inputs_hbm.shape
    width = freq_hbm.shape[1]
    total_features = width * ny * nc
    total_samples = rows * nx * nz
    held = nc * BLOCK
    members = ny * nx
    share = width // nx
    piece = width // PIECES
    half = PIECES // 2
    step_scale = BLOCK / total_samples
    ridge = 1.0 / BLOCK
    mx, mz = lax.axis_index("x"), lax.axis_index("z")
    my, mc = lax.axis_index("y"), lax.axis_index("core")
    other = lax.rem(mc + 1, nc)
    partner = {"core": other}

    def y_at(d):
        return lax.rem(my + d, ny)

    y_far_first = sorted(range(1, ny), key=lambda d: (-min(d, ny - d), d))

    def hops(d, n):
        return min(d, n - d)

    others = sorted(
        [(dy, dx) for dy in range(ny) for dx in range(nx) if (dy, dx) != (0, 0)],
        key=lambda o: (-hops(o[0], ny) - hops(o[1], nx), o),
    )
    mine = my * nx + mx

    def member(dy, dx):
        y, x = lax.rem(my + dy, ny), lax.rem(mx + dx, nx)
        return {"y": y, "x": x}, y * nx + x

    barrier = pltpu.get_barrier_semaphore()
    peers = [partner] + [member(dy, dx)[0] for dy, dx in others]
    peers += [{"z": lax.rem(mz + d, nz)} for d in range(1, nz)]
    for peer in peers:
        pl.semaphore_signal(barrier, inc=1, device_id=peer, device_id_type=MESH)
    loads = [
        pltpu.make_async_copy(src, dst, sem_in.at[k])
        for k, (src, dst) in enumerate(
            [
                (order_hbm, order_ref),
                (inputs_hbm, inputs_ref),
                (freq_hbm, freq.at[my, pl.ds(0, raw), :]),
                (phase_hbm, phases.at[my]),
                (target_hbm, target_ref),
            ]
        )
    ]
    for load in loads:
        load.start()
    loads[0].wait()

    own_order = order_ref[:, pl.ds(pl.multiple_of(my * held, held), held)]
    for part in range(rows // BLOCK):
        sample = lax.broadcasted_iota(jnp.int32, (BLOCK, held), 0) + part * BLOCK
        chosen[part * BLOCK : (part + 1) * BLOCK, :] = jnp.where(
            sample == own_order, 1.0, 0.0
        ).astype(BF16)
    line = lax.broadcasted_iota(jnp.int32, (128 - raw, held), 0)
    ones = jnp.where(line < 3, 1.0, 0.0)
    loads[1].wait()
    picked = jnp.concatenate([dot(inputs_ref[...], chosen[...]), ones], axis=0)
    picked_b[...] = jnp.transpose(picked).astype(BF16)

    for load in loads[2:]:
        load.wait()
    pl.semaphore_wait(barrier, len(peers))

    def remote(src, dst, out_sem, in_sem, device):
        return pltpu.make_async_remote_copy(
            src_ref=src,
            dst_ref=dst,
            send_sem=out_sem,
            recv_sem=in_sem,
            device_id=device,
            device_id_type=MESH,
        )

    def send(*args):
        copy = remote(*args)
        copy.start()
        return copy

    def cols(q):
        return pl.ds(pl.multiple_of(q * piece, piece), piece)

    def freq_piece(shard, q):
        return freq.at[shard, pl.ds(0, raw), cols(q)]

    y_right, y_left, y_far = y_at(1), y_at(ny - 1), y_at(2)
    started = []
    for d in y_far_first:
        started.append(
            send(phases.at[my], phases.at[my], out_phase.at[d], sem_phase.at[my], {"y": y_at(d)})
        )
    for i in range(PIECES):
        for q, out, y in ((i, out_right, y_right), ((i + half) % PIECES, out_left, y_left)):
            started.append(
                send(
                    freq_piece(my, q),
                    freq_piece(my, q),
                    out.at[q],
                    sem_piece.at[my, q],
                    {"y": y},
                )
            )
    wanted = jnp.sum(dot(three_rows(target_ref[...], 16), chosen[...]), axis=0, keepdims=True)

    amplitude = math.sqrt(2.0 / total_features)
    coefs = [-amplitude * v for v in SINE]
    gram[...] = jnp.zeros_like(gram)

    def make_piece(shard, q):
        freq[shard, raw:128, cols(q)] = three_rows(phases[shard, :, cols(q)], 128 - raw)
        for b in range(nc):
            block = slice(b * BLOCK, (b + 1) * BLOCK)
            angles = dot(picked_b[block, :], freq[shard, :, cols(q)])
            turns = angles * (0.5 / math.pi)
            wave = jnp.abs(turns - jnp.round(turns)) - 0.25
            square = wave * wave
            value = coefs[4]
            for c in (coefs[3], coefs[2], coefs[1], coefs[0]):
                value = value * square + c
            made = (value * wave).astype(BF16)
            phi[block, pl.ds(pl.multiple_of(shard * width + q * piece, piece), piece)] = made
            gram[b] += dot_t(made, made)

    def own_step(q, _):
        make_piece(my, q)
        return 0

    lax.fori_loop(0, PIECES, own_step, 0)

    def arrived(shard, q):
        remote(
            freq_piece(shard, q),
            freq_piece(shard, q),
            out_relay.at[0],
            sem_piece.at[shard, q],
            {"y": y_left},
        ).wait_recv()

    def phases_in(shard):
        remote(
            phases.at[shard], phases.at[shard], out_phase.at[0], sem_phase.at[shard], {"y": y_left}
        ).wait_recv()

    def relay(shard, q, y):
        started.append(
            send(
                freq_piece(shard, q),
                freq_piece(shard, q),
                out_relay.at[q],
                sem_piece.at[shard, q],
                {"y": y},
            )
        )

    for shard in (y_left, y_right, y_far):
        phases_in(shard)
    for i in range(PIECES):
        q, p = i, (i + half) % PIECES
        arrived(y_left, q)
        if i < half:
            relay(y_left, q, y_right)
        arrived(y_right, p)
        if i < half:
            relay(y_right, p, y_left)
        make_piece(y_left, q)
        make_piece(y_right, p)
    for i in range(half):
        for q in (i, i + half):
            arrived(y_far, q)
            make_piece(y_far, q)

    swap = send(gram.at[other], gram_in, out_swap.at[0], sem_gram.at[0], partner)
    row = lax.broadcasted_iota(jnp.int32, (BLOCK, BLOCK), 0)
    eye = jnp.where(row == lax.broadcasted_iota(jnp.int32, (BLOCK, BLOCK), 1), 1.0, 0.0)
    swap.wait()
    gram_in[...] = gram[mc] + gram_in[...] + eye

    scales = newton_schedule()
    first = 2.0 / (1.0 + TOP_EIGENVALUE)
    error = eye - first * gram_in[...]
    pair[0:BLOCK, :] = (scales[0] * first) * (eye + error)
    pair[BLOCK:, :] = (1.0 - scales[0]) * eye + scales[0] * dot_3(error, error)

    def newton(k, _):
        scale = jnp.float32(scales[1])
        for n in range(2, len(scales)):
            scale = jnp.where(k == n, jnp.float32(scales[n]), scale)
        product = dot_3(pair[...], pair[BLOCK:, :])
        pair[0:BLOCK, :] = scale * (pair[0:BLOCK, :] + product[0:BLOCK, :])
        pair[BLOCK:, :] = (1.0 - scale) * eye + scale * product[BLOCK:, :]
        return 0

    lax.fori_loop(1, len(scales), newton, 0)
    guess = pair[0:BLOCK, :]
    residual = eye - dot(gram_in[...], guess, HIGHEST)
    inverse[mc] = guess + dot_3(guess, residual)
    started.append(
        send(inverse.at[mc], inverse.at[mc], out_swap.at[1], sem_inverse.at[mc], partner)
    )
    remote(
        inverse.at[other], inverse.at[other], out_swap.at[1], sem_inverse.at[other], partner
    ).wait_recv()

    lanes = lax.broadcasted_iota(jnp.int32, (1, 128), 1)

    def exchange(buf, sem_in, sem_out, at, mine, count, axis):
        copies = []
        for d in range(1, count):
            copies.append(
                send(
                    buf.at[at, mine],
                    buf.at[at, mine],
                    sem_out.at[d],
                    sem_in.at[at, mine],
                    {axis: lax.rem(mine + d, count)},
                )
            )
        for d in range(1, count):
            source = lax.rem(mine + d, count)
            received(buf, sem_in, sem_out, at, source, {axis: source})
        return copies

    def received(buf, sem_in, sem_out, at, source, device):
        remote(
            buf.at[at, source],
            buf.at[at, source],
            sem_out.at[0],
            sem_in.at[at, source],
            device,
        ).wait_recv()

    def added(buf, at, count):
        value = buf[at, 0]
        for k in range(1, count):
            value = value + buf[at, k]
        return value

    def share_at(index, g, size):
        return pl.ds(pl.multiple_of(index * share + g * size, size), size)

    group = min(512, share)

    def weigh(index):
        done = []
        for g in range(share // group):
            at = share_at(index, g, group)
            total = jnp.zeros((16, group), F32)
            for t in range(held // 16):
                by = delta_c[t * 16 : (t + 1) * 16, :]
                by = jnp.concatenate([by] * (group // 128), axis=1)
                total = total + phi[t * 16 : (t + 1) * 16, at].astype(F32) * by
            done.append(jnp.sum(total, axis=0, keepdims=True))
        return jnp.concatenate(done, axis=1) * step_scale

    def add_margins(index, weight, first=False):
        used = weight.astype(BF16).astype(F32)
        tall = 64
        for t in range(held // tall):
            at = slice(t * tall, (t + 1) * tall)
            total = jnp.zeros((tall, 128), F32) if first else margin_c[at, :]
            for g in range(share // 128):
                columns = share_at(index, g, 128)
                total = total + phi[at, columns].astype(F32) * used[:, g * 128 : (g + 1) * 128]
            margin_c[at, :] = total

    def to_members(src, dst, out_sems, sem, at):
        copies = []
        for k, (dy, dx) in enumerate(others):
            device, _ = member(dy, dx)
            copies.append(send(src.at[at, mine], dst.at[at, mine], out_sems.at[k], sem.at[at, mine], device))
        return copies

    def from_member(buf, sem_in, sem_out, at, dy, dx):
        device, index = member(dy, dx)
        received(buf, sem_in, sem_out, at, index, device)
        return index

    def one_round(r, carry):
        alpha, margins, weights = carry
        rest = wanted - alpha - margins
        parts = []
        for b in range(nc):
            block = inverse[b] * rest[:, b * BLOCK : (b + 1) * BLOCK]
            parts.append(jnp.sum(block, axis=1, keepdims=True))
        column = jnp.broadcast_to(jnp.concatenate(parts, axis=0), (held, 128))
        delta_c[...] = column.astype(BF16).astype(F32)
        copies = []
        for k, (dy, dx) in enumerate(others):
            device, index = member(dy, dx)
            rs_send[r, k] = weigh(index)
            copies.append(
                send(rs_send.at[r, k], rs_recv.at[r, mine], out_rs.at[k], sem_rs.at[r, mine], device)
            )
        rs_recv[r, mine] = weigh(mine)
        turned = jnp.concatenate(
            [
                jnp.transpose(column[t * 128 : (t + 1) * 128, :])[0:1, :]
                for t in range(held // 128)
            ],
            axis=1,
        )
        alpha = alpha + turned
        for dy, dx in reversed(others):
            from_member(rs_recv, sem_rs, out_rs, r, dy, dx)
        part = added(rs_recv, r, members)
        if nz > 1:
            z_buf[r, mz] = part
            copies += exchange(z_buf, sem_z, out_z, r, mz, nz, "z")
            part = added(z_buf, r, nz)
        weights = weights + part
        ag_buf[r, mine] = weights
        copies += to_members(ag_buf, ag_buf, out_ag, sem_ag, r)
        add_margins(mine, weights, first=True)
        for dy, dx in reversed(others):
            index = from_member(ag_buf, sem_ag, out_ag, r, dy, dx)
            add_margins(index, ag_buf[r, index])
        row = jnp.concatenate(
            [
                jnp.sum(
                    jnp.transpose(margin_c[t * 128 : (t + 1) * 128, :]), axis=0, keepdims=True
                )
                for t in range(held // 128)
            ],
            axis=1,
        )
        margin_buf[r, mc] = row
        copies.append(
            send(
                margin_buf.at[r, mc],
                margin_buf.at[r, mc],
                out_margin.at[0],
                sem_margin.at[r, mc],
                partner,
            )
        )
        received(margin_buf, sem_margin, out_margin, r, other, partner)
        margins = added(margin_buf, r, nc)
        margin_rows[r] = margins
        alpha_rows[r] = alpha
        for copy in copies:
            copy.wait_send()
        return alpha, margins, weights

    zero = jnp.zeros((1, held), F32)
    alpha, _, _ = lax.fori_loop(
        0,
        ROUNDS,
        one_round,
        (zero, zero, jnp.zeros((1, share), F32)),
    )

    def in_lanes(values):
        line = jnp.zeros((1, 128), F32)
        for r, value in enumerate(values):
            line = jnp.where(lanes == r, jnp.sum(value, axis=1, keepdims=True), line)
        return line

    squares = in_lanes([(margin_rows[r] - wanted) ** 2 for r in range(ROUNDS)])
    gains = in_lanes(
        [alpha_rows[r] * wanted - 0.5 * alpha_rows[r] * alpha_rows[r] for r in range(ROUNDS)]
    )
    stat_g[0, mine] = jnp.concatenate([squares, gains], axis=0)
    copies = to_members(stat_g, stat_g, out_stat_g, sem_stat_g, 0)
    wholes = []
    for r in range(ROUNDS):
        whole = ag_buf[r, 0] * ag_buf[r, 0]
        for k in range(1, members):
            whole = whole + ag_buf[r, k] * ag_buf[r, k]
        wholes.append(whole)
    norm_buf[0, mc] = in_lanes(wholes)
    copies.append(
        send(norm_buf.at[0, mc], norm_buf.at[0, mc], out_swap.at[2], sem_norm.at[0, mc], partner)
    )
    dual_buf[0, my] = jnp.sum(dot_t(three_rows(alpha, 16), chosen[...]), axis=0, keepdims=True)
    for d in y_far_first:
        copies.append(
            send(
                dual_buf.at[0, my],
                dual_buf.at[0, my],
                out_dual.at[d],
                sem_dual.at[0, my],
                {"y": y_at(d)},
            )
        )
    weights_out[...] = jnp.concatenate(
        [ag_buf[ROUNDS - 1, my * nx + k] for k in range(nx)], axis=1
    )
    for dy, dx in reversed(others):
        from_member(stat_g, sem_stat_g, out_stat_g, 0, dy, dx)
    stats = added(stat_g, 0, members)
    if nz > 1:
        stat_z[0, mz] = stats
        copies += exchange(stat_z, sem_stat_z, out_stat_z, 0, mz, nz, "z")
        stats = added(stat_z, 0, nz)
    for d in range(1, ny):
        received(dual_buf, sem_dual, out_dual, 0, y_at(d), {"y": y_at(d)})
    duals_out[...] = added(dual_buf, 0, ny)
    received(norm_buf, sem_norm, out_swap, 0, other, partner)
    norms = added(norm_buf, 0, nc)
    primal = stats[0:1, :] / (2.0 * total_samples) + 0.5 * ridge * norms
    dual = stats[1:2, :] / total_samples - 0.5 * ridge * norms
    objectives_out[0:1, :] = primal[:, 0:ROUNDS]
    objectives_out[1:2, :] = dual[:, 0:ROUNDS]
    for copy in started + copies:
        copy.wait_send()


def copied(weights, duals, objectives, weights_out, duals_out, objectives_out):
    weights_out[...] = weights[...]
    duals_out[...] = duals[...]
    objectives_out[...] = objectives[...]


def on_device(sizes, inputs, frequencies, phases, targets, block_order):
    nx, nz, ny, nc = sizes
    rows, raw = inputs.shape
    width = frequencies.shape[1]
    held = nc * BLOCK
    members = ny * nx
    share = width // nx
    vmem = pl.BlockSpec(memory_space=pltpu.VMEM)
    dma = pltpu.SemaphoreType.DMA
    scratch = [
        pltpu.VMEM((raw, rows), BF16),
        pltpu.VMEM((1, rows), F32),
        pltpu.VMEM((1, rows), jnp.int32),
        pltpu.VMEM((held, 128), BF16),
        pltpu.VMEM((rows, held), BF16),
        pltpu.VMEM((ny, 128, width), BF16),
        pltpu.VMEM((ny, 1, width), F32),
        pltpu.VMEM((held, ny * width), BF16),
        pltpu.VMEM((nc, BLOCK, BLOCK), F32),
        pltpu.VMEM((BLOCK, BLOCK), F32),
        pltpu.VMEM((2 * BLOCK, BLOCK), F32),
        pltpu.VMEM((nc, BLOCK, BLOCK), F32),
        pltpu.VMEM((held, 128), F32),
        pltpu.VMEM((held, 128), F32),
        pltpu.VMEM((ROUNDS, 1, held), F32),
        pltpu.VMEM((ROUNDS, 1, held), F32),
        pltpu.VMEM((ROUNDS, members, 1, share), F32),
        pltpu.VMEM((ROUNDS, members, 1, share), F32),
        pltpu.VMEM((ROUNDS, nz, 1, share), F32),
        pltpu.VMEM((ROUNDS, members, 1, share), F32),
        pltpu.VMEM((ROUNDS, nc, 1, held), F32),
        pltpu.VMEM((1, nc, 1, 128), F32),
        pltpu.VMEM((1, ny, 1, rows), F32),
        pltpu.VMEM((1, members, 2, 128), F32),
        pltpu.VMEM((1, nz, 2, 128), F32),
        dma((5,)),
        dma((ny, PIECES)),
        dma((ny,)),
        dma((1,)),
        dma((nc,)),
        dma((ROUNDS, members)),
        dma((ROUNDS, nz)),
        dma((ROUNDS, members)),
        dma((ROUNDS, nc)),
        dma((1, nc)),
        dma((1, ny)),
        dma((1, members)),
        dma((1, nz)),
        dma((PIECES,)),
        dma((PIECES,)),
        dma((PIECES,)),
        dma((ny,)),
        dma((3,)),
        dma((members,)),
        dma((nz,)),
        dma((members,)),
        dma((1,)),
        dma((ny,)),
        dma((members,)),
        dma((nz,)),
    ]
    shapes = (
        jax.ShapeDtypeStruct((1, width), F32),
        jax.ShapeDtypeStruct((1, rows), F32),
        jax.ShapeDtypeStruct((2, ROUNDS), F32),
    )
    results = pl.pallas_call(
        functools.partial(kernel, sizes),
        out_shape=shapes,
        in_specs=[pl.BlockSpec(memory_space=pl.ANY)] * 5,
        out_specs=(vmem, vmem, vmem),
        scratch_shapes=scratch,
        compiler_params=pltpu.CompilerParams(
            collective_id=0, has_side_effects=True, vmem_limit_bytes=60 * 1024 * 1024
        ),
        name="cocoa",
    )(
        inputs.T,
        frequencies,
        phases.reshape(1, width),
        targets.reshape(1, rows),
        block_order.reshape(1, rows),
    )
    weights, duals, objectives = pl.pallas_call(
        copied,
        out_shape=shapes,
        in_specs=[vmem] * 3,
        out_specs=(vmem, vmem, vmem),
        name="results",
    )(*results)
    return weights.reshape(width), duals.reshape(rows), objectives.T


def solution(mesh):
    devices = mesh.devices
    samp, feat = mesh.shape["samp"], mesh.shape["feat"]
    nc = 2
    ny = feat // nc
    nx = math.gcd(samp, 4)
    nz = samp // nx
    torus = Mesh(devices.reshape(nx, nz, ny, nc), ("x", "z", "y", "core"))
    samp_axes, feat_axes = ("x", "z"), ("y", "core")
    in_specs = (
        P(samp_axes, None),
        P(None, feat_axes),
        P(feat_axes),
        P(samp_axes),
        P(samp_axes),
    )
    out_specs = (P(feat_axes), P(samp_axes), P())
    return jax.shard_map(
        functools.partial(on_device, (nx, nz, ny, nc)),
        mesh=torus,
        in_specs=in_specs,
        out_specs=out_specs,
        check_vma=False,
    )
```

```python
import functools
import math

import jax
import jax.numpy as jnp
from jax import lax
from jax.experimental import pallas as pl
from jax.experimental.pallas import tpu as pltpu
from jax.sharding import Mesh
from jax.sharding import PartitionSpec as P

BLOCK = 256
ROUNDS = 4
PIECES = 4
MESH = pl.DeviceIdType.MESH
HIGHEST = lax.Precision.HIGHEST
F32 = jnp.float32
BF16 = jnp.bfloat16

SINE = (
    6.283185273782525,
    -41.341677476882325,
    81.60223116950678,
    -76.57499088229173,
    39.71091059155359,
)
TOP_EIGENVALUE = 519.0


def newton_schedule():
    rho = (TOP_EIGENVALUE - 1.0) / (TOP_EIGENVALUE + 1.0)
    scales = []
    while rho > 1e-4:
        scale = 2.0 / (2.0 - rho * rho)
        rho = rho * rho * scale / 2.0
        scales.append(scale)
    return scales


def dot(a, b, precision=None):
    return lax.dot_general(
        a, b, (((1,), (0,)), ((), ())), precision=precision, preferred_element_type=F32
    )


def halves(value):
    high = value.astype(BF16)
    return high, (value - high.astype(F32)).astype(BF16)


def dot_3(a, b):
    a_high, a_low = halves(a)
    b_high, b_low = halves(b)
    return dot(a_high, b_high) + (dot(a_high, b_low) + dot(a_low, b_high))


def dot_t(a, b):
    return lax.dot_general(a, b, (((1,), (1,)), ((), ())), preferred_element_type=F32)


def three_rows(value, rows):
    high = value.astype(BF16).astype(F32)
    middle = (value - high).astype(BF16).astype(F32)
    low = value - high - middle
    shape = (rows, value.shape[1])
    row = lax.broadcasted_iota(jnp.int32, shape, 0)
    tile = jnp.where(row == 0, high, jnp.where(row == 1, middle, jnp.where(row == 2, low, 0.0)))
    return tile.astype(BF16)


def kernel(
    sizes,
    inputs_hbm,
    freq_hbm,
    phase_hbm,
    target_hbm,
    order_hbm,
    weights_out,
    duals_out,
    objectives_out,
    inputs_ref,
    target_ref,
    order_ref,
    picked_b,
    chosen,
    freq,
    phases,
    phi,
    gram,
    gram_in,
    pair,
    inverse,
    delta_c,
    margin_c,
    margin_rows,
    alpha_rows,
    rs_send,
    rs_recv,
    z_buf,
    ag_buf,
    margin_buf,
    norm_buf,
    dual_buf,
    stat_g,
    stat_z,
    sem_in,
    sem_piece,
    sem_phase,
    sem_gram,
    sem_inverse,
    sem_rs,
    sem_z,
    sem_ag,
    sem_margin,
    sem_norm,
    sem_dual,
    sem_stat_g,
    sem_stat_z,
    out_right,
    out_left,
    out_relay,
    out_phase,
    out_swap,
    out_rs,
    out_z,
    out_ag,
    out_margin,
    out_dual,
    out_stat_g,
    out_stat_z,
):
    nx, nz, ny, nc = sizes
    raw, rows = inputs_hbm.shape
    width = freq_hbm.shape[1]
    total_features = width * ny * nc
    total_samples = rows * nx * nz
    held = nc * BLOCK
    members = ny * nx
    share = width // nx
    piece = width // PIECES
    half = PIECES // 2
    step_scale = BLOCK / total_samples
    ridge = 1.0 / BLOCK
    mx, mz = lax.axis_index("x"), lax.axis_index("z")
    my, mc = lax.axis_index("y"), lax.axis_index("core")
    other = lax.rem(mc + 1, nc)
    partner = {"core": other}

    def y_at(d):
        return lax.rem(my + d, ny)

    y_far_first = sorted(range(1, ny), key=lambda d: (-min(d, ny - d), d))

    def hops(d, n):
        return min(d, n - d)

    others = sorted(
        [(dy, dx) for dy in range(ny) for dx in range(nx) if (dy, dx) != (0, 0)],
        key=lambda o: (-hops(o[0], ny) - hops(o[1], nx), o),
    )
    mine = my * nx + mx

    def member(dy, dx):
        y, x = lax.rem(my + dy, ny), lax.rem(mx + dx, nx)
        return {"y": y, "x": x}, y * nx + x

    barrier = pltpu.get_barrier_semaphore()
    peers = [partner] + [member(dy, dx)[0] for dy, dx in others]
    peers += [{"z": lax.rem(mz + d, nz)} for d in range(1, nz)]
    for peer in peers:
        pl.semaphore_signal(barrier, inc=1, device_id=peer, device_id_type=MESH)
    loads = [
        pltpu.make_async_copy(src, dst, sem_in.at[k])
        for k, (src, dst) in enumerate(
            [
                (order_hbm, order_ref),
                (inputs_hbm, inputs_ref),
                (freq_hbm, freq.at[my, pl.ds(0, raw), :]),
                (phase_hbm, phases.at[my]),
                (target_hbm, target_ref),
            ]
        )
    ]
    for load in loads:
        load.start()
    loads[0].wait()

    own_order = order_ref[:, pl.ds(pl.multiple_of(my * held, held), held)]
    for part in range(rows // BLOCK):
        sample = lax.broadcasted_iota(jnp.int32, (BLOCK, held), 0) + part * BLOCK
        chosen[part * BLOCK : (part + 1) * BLOCK, :] = jnp.where(
            sample == own_order, 1.0, 0.0
        ).astype(BF16)
    line = lax.broadcasted_iota(jnp.int32, (128 - raw, held), 0)
    ones = jnp.where(line < 3, 1.0, 0.0)
    loads[1].wait()
    picked = jnp.concatenate([dot(inputs_ref[...], chosen[...]), ones], axis=0)
    picked_b[...] = jnp.transpose(picked).astype(BF16)

    for load in loads[2:]:
        load.wait()
    pl.semaphore_wait(barrier, len(peers))

    def remote(src, dst, out_sem, in_sem, device):
        return pltpu.make_async_remote_copy(
            src_ref=src,
            dst_ref=dst,
            send_sem=out_sem,
            recv_sem=in_sem,
            device_id=device,
            device_id_type=MESH,
        )

    def send(*args):
        copy = remote(*args)
        copy.start()
        return copy

    def cols(q):
        return pl.ds(pl.multiple_of(q * piece, piece), piece)

    def freq_piece(shard, q):
        return freq.at[shard, pl.ds(0, raw), cols(q)]

    y_right, y_left, y_far = y_at(1), y_at(ny - 1), y_at(2)
    started = []
    for d in y_far_first:
        started.append(
            send(phases.at[my], phases.at[my], out_phase.at[d], sem_phase.at[my], {"y": y_at(d)})
        )
    for i in range(PIECES):
        for q, out, y in ((i, out_right, y_right), ((i + half) % PIECES, out_left, y_left)):
            started.append(
                send(
                    freq_piece(my, q),
                    freq_piece(my, q),
                    out.at[q],
                    sem_piece.at[my, q],
                    {"y": y},
                )
            )
    wanted = jnp.sum(dot(three_rows(target_ref[...], 16), chosen[...]), axis=0, keepdims=True)

    amplitude = math.sqrt(2.0 / total_features)
    coefs = [-amplitude * v for v in SINE]
    gram[...] = jnp.zeros_like(gram)

    def make_piece(shard, q):
        freq[shard, raw:128, cols(q)] = three_rows(phases[shard, :, cols(q)], 128 - raw)
        for b in range(nc):
            block = slice(b * BLOCK, (b + 1) * BLOCK)
            angles = dot(picked_b[block, :], freq[shard, :, cols(q)])
            turns = angles * (0.5 / math.pi)
            wave = jnp.abs(turns - jnp.round(turns)) - 0.25
            square = wave * wave
            value = coefs[4]
            for c in (coefs[3], coefs[2], coefs[1], coefs[0]):
                value = value * square + c
            made = (value * wave).astype(BF16)
            phi[block, pl.ds(pl.multiple_of(shard * width + q * piece, piece), piece)] = made
            gram[b] += dot_t(made, made)

    def own_step(q, _):
        make_piece(my, q)
        return 0

    lax.fori_loop(0, PIECES, own_step, 0)

    def arrived(shard, q):
        remote(
            freq_piece(shard, q),
            freq_piece(shard, q),
            out_relay.at[0],
            sem_piece.at[shard, q],
            {"y": y_left},
        ).wait_recv()

    def phases_in(shard):
        remote(
            phases.at[shard], phases.at[shard], out_phase.at[0], sem_phase.at[shard], {"y": y_left}
        ).wait_recv()

    def relay(shard, q, y):
        started.append(
            send(
                freq_piece(shard, q),
                freq_piece(shard, q),
                out_relay.at[q],
                sem_piece.at[shard, q],
                {"y": y},
            )
        )

    for shard in (y_left, y_right, y_far):
        phases_in(shard)
    for i in range(PIECES):
        q, p = i, (i + half) % PIECES
        arrived(y_left, q)
        if i < half:
            relay(y_left, q, y_right)
        arrived(y_right, p)
        if i < half:
            relay(y_right, p, y_left)
        make_piece(y_left, q)
        make_piece(y_right, p)
    for i in range(half):
        for q in (i, i + half):
            arrived(y_far, q)
            make_piece(y_far, q)

    swap = send(gram.at[other], gram_in, out_swap.at[0], sem_gram.at[0], partner)
    row = lax.broadcasted_iota(jnp.int32, (BLOCK, BLOCK), 0)
    eye = jnp.where(row == lax.broadcasted_iota(jnp.int32, (BLOCK, BLOCK), 1), 1.0, 0.0)
    swap.wait()
    gram_in[...] = gram[mc] + gram_in[...] + eye

    scales = newton_schedule()
    first = 2.0 / (1.0 + TOP_EIGENVALUE)
    error = eye - first * gram_in[...]
    pair[0:BLOCK, :] = (scales[0] * first) * (eye + error)
    pair[BLOCK:, :] = (1.0 - scales[0]) * eye + scales[0] * dot_3(error, error)

    def newton(k, _):
        scale = jnp.float32(scales[1])
        for n in range(2, len(scales)):
            scale = jnp.where(k == n, jnp.float32(scales[n]), scale)
        product = dot_3(pair[...], pair[BLOCK:, :])
        pair[0:BLOCK, :] = scale * (pair[0:BLOCK, :] + product[0:BLOCK, :])
        pair[BLOCK:, :] = (1.0 - scale) * eye + scale * product[BLOCK:, :]
        return 0

    lax.fori_loop(1, len(scales), newton, 0)
    guess = pair[0:BLOCK, :]
    residual = eye - dot(gram_in[...], guess, HIGHEST)
    inverse[mc] = guess + dot_3(guess, residual)
    started.append(
        send(inverse.at[mc], inverse.at[mc], out_swap.at[1], sem_inverse.at[mc], partner)
    )
    remote(
        inverse.at[other], inverse.at[other], out_swap.at[1], sem_inverse.at[other], partner
    ).wait_recv()

    lanes = lax.broadcasted_iota(jnp.int32, (1, 128), 1)

    def exchange(buf, sem_in, sem_out, at, mine, count, axis):
        copies = []
        far_first = sorted(range(1, count), key=lambda d: -hops(d, count))
        for d in far_first:
            copies.append(
                send(
                    buf.at[at, mine],
                    buf.at[at, mine],
                    sem_out.at[d],
                    sem_in.at[at, mine],
                    {axis: lax.rem(mine + d, count)},
                )
            )
        for d in reversed(far_first):
            source = lax.rem(mine + d, count)
            received(buf, sem_in, sem_out, at, source, {axis: source})
        return copies

    def received(buf, sem_in, sem_out, at, source, device):
        remote(
            buf.at[at, source],
            buf.at[at, source],
            sem_out.at[0],
            sem_in.at[at, source],
            device,
        ).wait_recv()

    def added(buf, at, count):
        value = buf[at, 0]
        for k in range(1, count):
            value = value + buf[at, k]
        return value

    def share_at(index, g, size):
        return pl.ds(pl.multiple_of(index * share + g * size, size), size)

    group = min(512, share)

    def weigh(index):
        done = []
        for g in range(share // group):
            at = share_at(index, g, group)
            total = jnp.zeros((16, group), F32)
            for t in range(held // 16):
                by = delta_c[t * 16 : (t + 1) * 16, :]
                by = jnp.concatenate([by] * (group // 128), axis=1)
                total = total + phi[t * 16 : (t + 1) * 16, at].astype(F32) * by
            done.append(jnp.sum(total, axis=0, keepdims=True))
        return jnp.concatenate(done, axis=1) * step_scale

    def add_margins(index, weight, first=False):
        used = weight.astype(BF16).astype(F32)
        tall = 64
        for t in range(held // tall):
            at = slice(t * tall, (t + 1) * tall)
            total = jnp.zeros((tall, 128), F32) if first else margin_c[at, :]
            for g in range(share // 128):
                columns = share_at(index, g, 128)
                total = total + phi[at, columns].astype(F32) * used[:, g * 128 : (g + 1) * 128]
            margin_c[at, :] = total

    def to_members(src, dst, out_sems, sem, at):
        copies = []
        for k, (dy, dx) in enumerate(others):
            device, _ = member(dy, dx)
            copies.append(send(src.at[at, mine], dst.at[at, mine], out_sems.at[k], sem.at[at, mine], device))
        return copies

    def from_member(buf, sem_in, sem_out, at, dy, dx):
        device, index = member(dy, dx)
        received(buf, sem_in, sem_out, at, index, device)
        return index

    def one_round(r, carry):
        alpha, margins, weights = carry
        rest = wanted - alpha - margins
        parts = []
        for b in range(nc):
            block = inverse[b] * rest[:, b * BLOCK : (b + 1) * BLOCK]
            parts.append(jnp.sum(block, axis=1, keepdims=True))
        column = jnp.broadcast_to(jnp.concatenate(parts, axis=0), (held, 128))
        delta_c[...] = column.astype(BF16).astype(F32)
        copies = []
        for k, (dy, dx) in enumerate(others):
            device, index = member(dy, dx)
            rs_send[r, k] = weigh(index)
            copies.append(
                send(rs_send.at[r, k], rs_recv.at[r, mine], out_rs.at[k], sem_rs.at[r, mine], device)
            )
        rs_recv[r, mine] = weigh(mine)
        turned = jnp.concatenate(
            [
                jnp.transpose(column[t * 128 : (t + 1) * 128, :])[0:1, :]
                for t in range(held // 128)
            ],
            axis=1,
        )
        alpha = alpha + turned
        for dy, dx in reversed(others):
            from_member(rs_recv, sem_rs, out_rs, r, dy, dx)
        part = added(rs_recv, r, members)
        if nz > 1:
            z_buf[r, mz] = part
            copies += exchange(z_buf, sem_z, out_z, r, mz, nz, "z")
            part = added(z_buf, r, nz)
        weights = weights + part
        ag_buf[r, mine] = weights
        copies += to_members(ag_buf, ag_buf, out_ag, sem_ag, r)
        add_margins(mine, weights, first=True)
        for dy, dx in reversed(others):
            index = from_member(ag_buf, sem_ag, out_ag, r, dy, dx)
            add_margins(index, ag_buf[r, index])
        row = jnp.concatenate(
            [
                jnp.sum(
                    jnp.transpose(margin_c[t * 128 : (t + 1) * 128, :]), axis=0, keepdims=True
                )
                for t in range(held // 128)
            ],
            axis=1,
        )
        margin_buf[r, mc] = row
        copies.append(
            send(
                margin_buf.at[r, mc],
                margin_buf.at[r, mc],
                out_margin.at[0],
                sem_margin.at[r, mc],
                partner,
            )
        )
        received(margin_buf, sem_margin, out_margin, r, other, partner)
        margins = added(margin_buf, r, nc)
        margin_rows[r] = margins
        alpha_rows[r] = alpha
        for copy in copies:
            copy.wait_send()
        return alpha, margins, weights

    zero = jnp.zeros((1, held), F32)
    alpha, _, _ = lax.fori_loop(
        0,
        ROUNDS,
        one_round,
        (zero, zero, jnp.zeros((1, share), F32)),
    )

    def in_lanes(values):
        line = jnp.zeros((1, 128), F32)
        for r, value in enumerate(values):
            line = jnp.where(lanes == r, jnp.sum(value, axis=1, keepdims=True), line)
        return line

    squares = in_lanes([(margin_rows[r] - wanted) ** 2 for r in range(ROUNDS)])
    gains = in_lanes(
        [alpha_rows[r] * wanted - 0.5 * alpha_rows[r] * alpha_rows[r] for r in range(ROUNDS)]
    )
    stat_g[0, mine] = jnp.concatenate([squares, gains], axis=0)
    copies = to_members(stat_g, stat_g, out_stat_g, sem_stat_g, 0)
    wholes = []
    for r in range(ROUNDS):
        whole = ag_buf[r, 0] * ag_buf[r, 0]
        for k in range(1, members):
            whole = whole + ag_buf[r, k] * ag_buf[r, k]
        wholes.append(whole)
    norm_buf[0, mc] = in_lanes(wholes)
    copies.append(
        send(norm_buf.at[0, mc], norm_buf.at[0, mc], out_swap.at[2], sem_norm.at[0, mc], partner)
    )
    dual_buf[0, my] = jnp.sum(dot_t(three_rows(alpha, 16), chosen[...]), axis=0, keepdims=True)
    for d in y_far_first:
        copies.append(
            send(
                dual_buf.at[0, my],
                dual_buf.at[0, my],
                out_dual.at[d],
                sem_dual.at[0, my],
                {"y": y_at(d)},
            )
        )
    weights_out[...] = jnp.concatenate(
        [ag_buf[ROUNDS - 1, my * nx + k] for k in range(nx)], axis=1
    )
    for dy, dx in reversed(others):
        from_member(stat_g, sem_stat_g, out_stat_g, 0, dy, dx)
    stats = added(stat_g, 0, members)
    if nz > 1:
        stat_z[0, mz] = stats
        copies += exchange(stat_z, sem_stat_z, out_stat_z, 0, mz, nz, "z")
        stats = added(stat_z, 0, nz)
    for d in range(1, ny):
        received(dual_buf, sem_dual, out_dual, 0, y_at(d), {"y": y_at(d)})
    duals_out[...] = added(dual_buf, 0, ny)
    received(norm_buf, sem_norm, out_swap, 0, other, partner)
    norms = added(norm_buf, 0, nc)
    primal = stats[0:1, :] / (2.0 * total_samples) + 0.5 * ridge * norms
    dual = stats[1:2, :] / total_samples - 0.5 * ridge * norms
    objectives_out[0:1, :] = primal[:, 0:ROUNDS]
    objectives_out[1:2, :] = dual[:, 0:ROUNDS]
    for copy in started + copies:
        copy.wait_send()


def copied(weights, duals, objectives, weights_out, duals_out, objectives_out):
    weights_out[...] = weights[...]
    duals_out[...] = duals[...]
    objectives_out[...] = objectives[...]


def on_device(sizes, inputs, frequencies, phases, targets, block_order):
    nx, nz, ny, nc = sizes
    rows, raw = inputs.shape
    width = frequencies.shape[1]
    held = nc * BLOCK
    members = ny * nx
    share = width // nx
    vmem = pl.BlockSpec(memory_space=pltpu.VMEM)
    dma = pltpu.SemaphoreType.DMA
    scratch = [
        pltpu.VMEM((raw, rows), BF16),
        pltpu.VMEM((1, rows), F32),
        pltpu.VMEM((1, rows), jnp.int32),
        pltpu.VMEM((held, 128), BF16),
        pltpu.VMEM((rows, held), BF16),
        pltpu.VMEM((ny, 128, width), BF16),
        pltpu.VMEM((ny, 1, width), F32),
        pltpu.VMEM((held, ny * width), BF16),
        pltpu.VMEM((nc, BLOCK, BLOCK), F32),
        pltpu.VMEM((BLOCK, BLOCK), F32),
        pltpu.VMEM((2 * BLOCK, BLOCK), F32),
        pltpu.VMEM((nc, BLOCK, BLOCK), F32),
        pltpu.VMEM((held, 128), F32),
        pltpu.VMEM((held, 128), F32),
        pltpu.VMEM((ROUNDS, 1, held), F32),
        pltpu.VMEM((ROUNDS, 1, held), F32),
        pltpu.VMEM((ROUNDS, members, 1, share), F32),
        pltpu.VMEM((ROUNDS, members, 1, share), F32),
        pltpu.VMEM((ROUNDS, nz, 1, share), F32),
        pltpu.VMEM((ROUNDS, members, 1, share), F32),
        pltpu.VMEM((ROUNDS, nc, 1, held), F32),
        pltpu.VMEM((1, nc, 1, 128), F32),
        pltpu.VMEM((1, ny, 1, rows), F32),
        pltpu.VMEM((1, members, 2, 128), F32),
        pltpu.VMEM((1, nz, 2, 128), F32),
        dma((5,)),
        dma((ny, PIECES)),
        dma((ny,)),
        dma((1,)),
        dma((nc,)),
        dma((ROUNDS, members)),
        dma((ROUNDS, nz)),
        dma((ROUNDS, members)),
        dma((ROUNDS, nc)),
        dma((1, nc)),
        dma((1, ny)),
        dma((1, members)),
        dma((1, nz)),
        dma((PIECES,)),
        dma((PIECES,)),
        dma((PIECES,)),
        dma((ny,)),
        dma((3,)),
        dma((members,)),
        dma((nz,)),
        dma((members,)),
        dma((1,)),
        dma((ny,)),
        dma((members,)),
        dma((nz,)),
    ]
    shapes = (
        jax.ShapeDtypeStruct((1, width), F32),
        jax.ShapeDtypeStruct((1, rows), F32),
        jax.ShapeDtypeStruct((2, ROUNDS), F32),
    )
    results = pl.pallas_call(
        functools.partial(kernel, sizes),
        out_shape=shapes,
        in_specs=[pl.BlockSpec(memory_space=pl.ANY)] * 5,
        out_specs=(vmem, vmem, vmem),
        scratch_shapes=scratch,
        compiler_params=pltpu.CompilerParams(
            collective_id=0, has_side_effects=True, vmem_limit_bytes=60 * 1024 * 1024
        ),
        name="cocoa",
    )(
        inputs.T,
        frequencies,
        phases.reshape(1, width),
        targets.reshape(1, rows),
        block_order.reshape(1, rows),
    )
    weights, duals, objectives = pl.pallas_call(
        copied,
        out_shape=shapes,
        in_specs=[vmem] * 3,
        out_specs=(vmem, vmem, vmem),
        name="results",
    )(*results)
    return weights.reshape(width), duals.reshape(rows), objectives.T


def solution(mesh):
    devices = mesh.devices
    samp, feat = mesh.shape["samp"], mesh.shape["feat"]
    nc = 2
    ny = feat // nc
    nx = math.gcd(samp, 4)
    nz = samp // nx
    torus = Mesh(devices.reshape(nx, nz, ny, nc), ("x", "z", "y", "core"))
    samp_axes, feat_axes = ("x", "z"), ("y", "core")
    in_specs = (
        P(samp_axes, None),
        P(None, feat_axes),
        P(feat_axes),
        P(samp_axes),
        P(samp_axes),
    )
    out_specs = (P(feat_axes), P(samp_axes), P())
    return jax.shard_map(
        functools.partial(on_device, (nx, nz, ny, nc)),
        mesh=torus,
        in_specs=in_specs,
        out_specs=out_specs,
        check_vma=False,
    )
```

```python
import functools
import math

import jax
import jax.numpy as jnp
from jax import lax
from jax.experimental import pallas as pl
from jax.experimental.pallas import tpu as pltpu
from jax.sharding import Mesh
from jax.sharding import PartitionSpec as P

BLOCK = 256
ROUNDS = 4
PIECES = 4
MESH = pl.DeviceIdType.MESH
HIGHEST = lax.Precision.HIGHEST
F32 = jnp.float32
BF16 = jnp.bfloat16

SINE = (
    6.283185273782525,
    -41.341677476882325,
    81.60223116950678,
    -76.57499088229173,
    39.71091059155359,
)
TOP_EIGENVALUE = 519.0


def newton_schedule():
    rho = (TOP_EIGENVALUE - 1.0) / (TOP_EIGENVALUE + 1.0)
    scales = []
    while rho > 1e-4:
        scale = 2.0 / (2.0 - rho * rho)
        rho = rho * rho * scale / 2.0
        scales.append(scale)
    return scales


def dot(a, b, precision=None):
    return lax.dot_general(
        a, b, (((1,), (0,)), ((), ())), precision=precision, preferred_element_type=F32
    )


def halves(value):
    high = value.astype(BF16)
    return high, (value - high.astype(F32)).astype(BF16)


def dot_3(a, b):
    a_high, a_low = halves(a)
    b_high, b_low = halves(b)
    return dot(a_high, b_high) + (dot(a_high, b_low) + dot(a_low, b_high))


def dot_t(a, b):
    return lax.dot_general(a, b, (((1,), (1,)), ((), ())), preferred_element_type=F32)


def three_rows(value, rows):
    high = value.astype(BF16).astype(F32)
    middle = (value - high).astype(BF16).astype(F32)
    low = value - high - middle
    shape = (rows, value.shape[1])
    row = lax.broadcasted_iota(jnp.int32, shape, 0)
    tile = jnp.where(row == 0, high, jnp.where(row == 1, middle, jnp.where(row == 2, low, 0.0)))
    return tile.astype(BF16)


def kernel(
    sizes,
    inputs_hbm,
    freq_hbm,
    phase_hbm,
    target_hbm,
    order_hbm,
    weights_out,
    duals_out,
    objectives_out,
    inputs_ref,
    target_ref,
    order_ref,
    picked_b,
    chosen,
    freq,
    phases,
    phi,
    gram,
    gram_in,
    pair,
    inverse,
    delta_c,
    margin_c,
    margin_rows,
    alpha_rows,
    rs_send,
    rs_recv,
    z_buf,
    ag_buf,
    margin_buf,
    norm_buf,
    dual_buf,
    stat_g,
    stat_z,
    sem_in,
    sem_piece,
    sem_phase,
    sem_gram,
    sem_inverse,
    sem_rs,
    sem_z,
    sem_ag,
    sem_margin,
    sem_norm,
    sem_dual,
    sem_stat_g,
    sem_stat_z,
    out_right,
    out_left,
    out_relay,
    out_phase,
    out_swap,
    out_rs,
    out_z,
    out_ag,
    out_margin,
    out_dual,
    out_stat_g,
    out_stat_z,
):
    nx, nz, ny, nc = sizes
    raw, rows = inputs_hbm.shape
    width = freq_hbm.shape[1]
    total_features = width * ny * nc
    total_samples = rows * nx * nz
    held = nc * BLOCK
    members = ny * nx
    share = width // nx
    piece = width // PIECES
    half = PIECES // 2
    step_scale = BLOCK / total_samples
    ridge = 1.0 / BLOCK
    mx, mz = lax.axis_index("x"), lax.axis_index("z")
    my, mc = lax.axis_index("y"), lax.axis_index("core")
    other = lax.rem(mc + 1, nc)
    partner = {"core": other}

    def y_at(d):
        return lax.rem(my + d, ny)

    y_far_first = sorted(range(1, ny), key=lambda d: (-min(d, ny - d), d))

    def hops(d, n):
        return min(d, n - d)

    others = sorted(
        [(dy, dx) for dy in range(ny) for dx in range(nx) if (dy, dx) != (0, 0)],
        key=lambda o: (-hops(o[0], ny) - hops(o[1], nx), o),
    )
    mine = my * nx + mx

    def member(dy, dx):
        y, x = lax.rem(my + dy, ny), lax.rem(mx + dx, nx)
        return {"y": y, "x": x}, y * nx + x

    barrier = pltpu.get_barrier_semaphore()
    peers = [partner] + [member(dy, dx)[0] for dy, dx in others]
    peers += [{"z": lax.rem(mz + d, nz)} for d in range(1, nz)]
    for peer in peers:
        pl.semaphore_signal(barrier, inc=1, device_id=peer, device_id_type=MESH)
    loads = [
        pltpu.make_async_copy(src, dst, sem_in.at[k])
        for k, (src, dst) in enumerate(
            [
                (order_hbm, order_ref),
                (inputs_hbm, inputs_ref),
                (freq_hbm, freq.at[my, pl.ds(0, raw), :]),
                (phase_hbm, phases.at[my]),
                (target_hbm, target_ref),
            ]
        )
    ]
    for load in loads:
        load.start()
    loads[0].wait()

    own_order = order_ref[:, pl.ds(pl.multiple_of(my * held, held), held)]
    for part in range(rows // BLOCK):
        sample = lax.broadcasted_iota(jnp.int32, (BLOCK, held), 0) + part * BLOCK
        chosen[part * BLOCK : (part + 1) * BLOCK, :] = jnp.where(
            sample == own_order, 1.0, 0.0
        ).astype(BF16)
    line = lax.broadcasted_iota(jnp.int32, (128 - raw, held), 0)
    ones = jnp.where(line < 3, 1.0, 0.0)
    loads[1].wait()
    picked = jnp.concatenate([dot(inputs_ref[...], chosen[...]), ones], axis=0)
    picked_b[...] = jnp.transpose(picked).astype(BF16)

    for load in loads[2:]:
        load.wait()
    pl.semaphore_wait(barrier, len(peers))

    def remote(src, dst, out_sem, in_sem, device):
        return pltpu.make_async_remote_copy(
            src_ref=src,
            dst_ref=dst,
            send_sem=out_sem,
            recv_sem=in_sem,
            device_id=device,
            device_id_type=MESH,
        )

    def send(*args):
        copy = remote(*args)
        copy.start()
        return copy

    def cols(q):
        return pl.ds(pl.multiple_of(q * piece, piece), piece)

    def freq_piece(shard, q):
        return freq.at[shard, pl.ds(0, raw), cols(q)]

    y_right, y_left, y_far = y_at(1), y_at(ny - 1), y_at(2)
    started = []
    for d in y_far_first:
        started.append(
            send(phases.at[my], phases.at[my], out_phase.at[d], sem_phase.at[my], {"y": y_at(d)})
        )
    for i in range(PIECES):
        for q, out, y in ((i, out_right, y_right), ((i + half) % PIECES, out_left, y_left)):
            started.append(
                send(
                    freq_piece(my, q),
                    freq_piece(my, q),
                    out.at[q],
                    sem_piece.at[my, q],
                    {"y": y},
                )
            )

    amplitude = math.sqrt(2.0 / total_features)
    coefs = [-amplitude * v for v in SINE]
    gram[...] = jnp.zeros_like(gram)

    def make_piece(shard, q):
        freq[shard, raw:128, cols(q)] = three_rows(phases[shard, :, cols(q)], 128 - raw)
        for b in range(nc):
            block = slice(b * BLOCK, (b + 1) * BLOCK)
            angles = dot(picked_b[block, :], freq[shard, :, cols(q)])
            turns = angles * (0.5 / math.pi)
            wave = jnp.abs(turns - jnp.round(turns)) - 0.25
            square = wave * wave
            value = coefs[4]
            for c in (coefs[3], coefs[2], coefs[1], coefs[0]):
                value = value * square + c
            made = (value * wave).astype(BF16)
            phi[block, pl.ds(pl.multiple_of(shard * width + q * piece, piece), piece)] = made
            gram[b] += dot_t(made, made)

    def own_step(q, _):
        make_piece(my, q)
        return 0

    lax.fori_loop(0, PIECES, own_step, 0)

    def arrived(shard, q):
        remote(
            freq_piece(shard, q),
            freq_piece(shard, q),
            out_relay.at[0],
            sem_piece.at[shard, q],
            {"y": y_left},
        ).wait_recv()

    def phases_in(shard):
        remote(
            phases.at[shard], phases.at[shard], out_phase.at[0], sem_phase.at[shard], {"y": y_left}
        ).wait_recv()

    def relay(shard, q, y):
        started.append(
            send(
                freq_piece(shard, q),
                freq_piece(shard, q),
                out_relay.at[q],
                sem_piece.at[shard, q],
                {"y": y},
            )
        )

    for shard in (y_left, y_right, y_far):
        phases_in(shard)
    for i in range(PIECES):
        q, p = i, (i + half) % PIECES
        arrived(y_left, q)
        if i < half:
            relay(y_left, q, y_right)
        arrived(y_right, p)
        if i < half:
            relay(y_right, p, y_left)
        make_piece(y_left, q)
        make_piece(y_right, p)
    for i in range(half):
        for q in (i, i + half):
            arrived(y_far, q)
            make_piece(y_far, q)

    swap = send(gram.at[other], gram_in, out_swap.at[0], sem_gram.at[0], partner)
    wanted = jnp.sum(dot(three_rows(target_ref[...], 16), chosen[...]), axis=0, keepdims=True)
    row = lax.broadcasted_iota(jnp.int32, (BLOCK, BLOCK), 0)
    eye = jnp.where(row == lax.broadcasted_iota(jnp.int32, (BLOCK, BLOCK), 1), 1.0, 0.0)
    swap.wait()
    gram_in[...] = gram[mc] + gram_in[...] + eye

    scales = newton_schedule()
    first = 2.0 / (1.0 + TOP_EIGENVALUE)
    error = eye - first * gram_in[...]
    pair[0:BLOCK, :] = (scales[0] * first) * (eye + error)
    pair[BLOCK:, :] = (1.0 - scales[0]) * eye + scales[0] * dot_3(error, error)

    def newton(k, _):
        scale = jnp.float32(scales[1])
        for n in range(2, len(scales)):
            scale = jnp.where(k == n, jnp.float32(scales[n]), scale)
        product = dot_3(pair[...], pair[BLOCK:, :])
        pair[0:BLOCK, :] = scale * (pair[0:BLOCK, :] + product[0:BLOCK, :])
        pair[BLOCK:, :] = (1.0 - scale) * eye + scale * product[BLOCK:, :]
        return 0

    lax.fori_loop(1, len(scales), newton, 0)
    guess = pair[0:BLOCK, :]
    residual = eye - dot(gram_in[...], guess, HIGHEST)
    inverse[mc] = guess + dot_3(guess, residual)
    started.append(
        send(inverse.at[mc], inverse.at[mc], out_swap.at[1], sem_inverse.at[mc], partner)
    )
    remote(
        inverse.at[other], inverse.at[other], out_swap.at[1], sem_inverse.at[other], partner
    ).wait_recv()

    lanes = lax.broadcasted_iota(jnp.int32, (1, 128), 1)

    def exchange(buf, sem_in, sem_out, at, mine, count, axis):
        copies = []
        far_first = sorted(range(1, count), key=lambda d: -hops(d, count))
        for d in far_first:
            copies.append(
                send(
                    buf.at[at, mine],
                    buf.at[at, mine],
                    sem_out.at[d],
                    sem_in.at[at, mine],
                    {axis: lax.rem(mine + d, count)},
                )
            )
        for d in reversed(far_first):
            source = lax.rem(mine + d, count)
            received(buf, sem_in, sem_out, at, source, {axis: source})
        return copies

    def received(buf, sem_in, sem_out, at, source, device):
        remote(
            buf.at[at, source],
            buf.at[at, source],
            sem_out.at[0],
            sem_in.at[at, source],
            device,
        ).wait_recv()

    def added(buf, at, count):
        value = buf[at, 0]
        for k in range(1, count):
            value = value + buf[at, k]
        return value

    def share_at(index, g, size):
        return pl.ds(pl.multiple_of(index * share + g * size, size), size)

    group = min(512, share)

    def weigh(index):
        done = []
        for g in range(share // group):
            at = share_at(index, g, group)
            total = jnp.zeros((16, group), F32)
            for t in range(held // 16):
                by = delta_c[t * 16 : (t + 1) * 16, :]
                by = jnp.concatenate([by] * (group // 128), axis=1)
                total = total + phi[t * 16 : (t + 1) * 16, at].astype(F32) * by
            done.append(jnp.sum(total, axis=0, keepdims=True))
        return jnp.concatenate(done, axis=1) * step_scale

    def add_margins(index, weight, first=False):
        used = weight.astype(BF16).astype(F32)
        tall = 64
        for t in range(held // tall):
            at = slice(t * tall, (t + 1) * tall)
            total = jnp.zeros((tall, 128), F32) if first else margin_c[at, :]
            for g in range(share // 128):
                columns = share_at(index, g, 128)
                total = total + phi[at, columns].astype(F32) * used[:, g * 128 : (g + 1) * 128]
            margin_c[at, :] = total

    def to_members(src, dst, out_sems, sem, at):
        copies = []
        for k, (dy, dx) in enumerate(others):
            device, _ = member(dy, dx)
            copies.append(send(src.at[at, mine], dst.at[at, mine], out_sems.at[k], sem.at[at, mine], device))
        return copies

    def from_member(buf, sem_in, sem_out, at, dy, dx):
        device, index = member(dy, dx)
        received(buf, sem_in, sem_out, at, index, device)
        return index

    def one_round(r, carry):
        alpha, margins, weights = carry
        rest = wanted - alpha - margins
        parts = []
        for b in range(nc):
            block = inverse[b] * rest[:, b * BLOCK : (b + 1) * BLOCK]
            parts.append(jnp.sum(block, axis=1, keepdims=True))
        column = jnp.broadcast_to(jnp.concatenate(parts, axis=0), (held, 128))
        delta_c[...] = column.astype(BF16).astype(F32)
        copies = []
        for k, (dy, dx) in enumerate(others):
            device, index = member(dy, dx)
            rs_send[r, k] = weigh(index)
            copies.append(
                send(rs_send.at[r, k], rs_recv.at[r, mine], out_rs.at[k], sem_rs.at[r, mine], device)
            )
        rs_recv[r, mine] = weigh(mine)
        turned = jnp.concatenate(
            [
                jnp.transpose(column[t * 128 : (t + 1) * 128, :])[0:1, :]
                for t in range(held // 128)
            ],
            axis=1,
        )
        alpha = alpha + turned
        for dy, dx in reversed(others):
            from_member(rs_recv, sem_rs, out_rs, r, dy, dx)
        part = added(rs_recv, r, members)
        if nz > 1:
            z_buf[r, mz] = part
            copies += exchange(z_buf, sem_z, out_z, r, mz, nz, "z")
            part = added(z_buf, r, nz)
        weights = weights + part
        ag_buf[r, mine] = weights
        copies += to_members(ag_buf, ag_buf, out_ag, sem_ag, r)
        add_margins(mine, weights, first=True)
        for dy, dx in reversed(others):
            index = from_member(ag_buf, sem_ag, out_ag, r, dy, dx)
            add_margins(index, ag_buf[r, index])
        row = jnp.concatenate(
            [
                jnp.sum(
                    jnp.transpose(margin_c[t * 128 : (t + 1) * 128, :]), axis=0, keepdims=True
                )
                for t in range(held // 128)
            ],
            axis=1,
        )
        margin_buf[r, mc] = row
        copies.append(
            send(
                margin_buf.at[r, mc],
                margin_buf.at[r, mc],
                out_margin.at[0],
                sem_margin.at[r, mc],
                partner,
            )
        )
        received(margin_buf, sem_margin, out_margin, r, other, partner)
        margins = added(margin_buf, r, nc)
        margin_rows[r] = margins
        alpha_rows[r] = alpha
        for copy in copies:
            copy.wait_send()
        return alpha, margins, weights

    zero = jnp.zeros((1, held), F32)
    alpha, _, _ = lax.fori_loop(
        0,
        ROUNDS,
        one_round,
        (zero, zero, jnp.zeros((1, share), F32)),
    )

    def in_lanes(values):
        line = jnp.zeros((1, 128), F32)
        for r, value in enumerate(values):
            line = jnp.where(lanes == r, jnp.sum(value, axis=1, keepdims=True), line)
        return line

    squares = in_lanes([(margin_rows[r] - wanted) ** 2 for r in range(ROUNDS)])
    gains = in_lanes(
        [alpha_rows[r] * wanted - 0.5 * alpha_rows[r] * alpha_rows[r] for r in range(ROUNDS)]
    )
    stat_g[0, mine] = jnp.concatenate([squares, gains], axis=0)
    copies = to_members(stat_g, stat_g, out_stat_g, sem_stat_g, 0)
    wholes = []
    for r in range(ROUNDS):
        whole = ag_buf[r, 0] * ag_buf[r, 0]
        for k in range(1, members):
            whole = whole + ag_buf[r, k] * ag_buf[r, k]
        wholes.append(whole)
    norm_buf[0, mc] = in_lanes(wholes)
    copies.append(
        send(norm_buf.at[0, mc], norm_buf.at[0, mc], out_swap.at[2], sem_norm.at[0, mc], partner)
    )
    dual_buf[0, my] = jnp.sum(dot_t(three_rows(alpha, 16), chosen[...]), axis=0, keepdims=True)
    for d in y_far_first:
        copies.append(
            send(
                dual_buf.at[0, my],
                dual_buf.at[0, my],
                out_dual.at[d],
                sem_dual.at[0, my],
                {"y": y_at(d)},
            )
        )
    weights_out[...] = jnp.concatenate(
        [ag_buf[ROUNDS - 1, my * nx + k] for k in range(nx)], axis=1
    )
    for dy, dx in reversed(others):
        from_member(stat_g, sem_stat_g, out_stat_g, 0, dy, dx)
    stats = added(stat_g, 0, members)
    if nz > 1:
        stat_z[0, mz] = stats
        copies += exchange(stat_z, sem_stat_z, out_stat_z, 0, mz, nz, "z")
        stats = added(stat_z, 0, nz)
    for d in range(1, ny):
        received(dual_buf, sem_dual, out_dual, 0, y_at(d), {"y": y_at(d)})
    duals_out[...] = added(dual_buf, 0, ny)
    received(norm_buf, sem_norm, out_swap, 0, other, partner)
    norms = added(norm_buf, 0, nc)
    primal = stats[0:1, :] / (2.0 * total_samples) + 0.5 * ridge * norms
    dual = stats[1:2, :] / total_samples - 0.5 * ridge * norms
    objectives_out[0:1, :] = primal[:, 0:ROUNDS]
    objectives_out[1:2, :] = dual[:, 0:ROUNDS]
    for copy in started + copies:
        copy.wait_send()


def copied(weights, duals, objectives, weights_out, duals_out, objectives_out):
    weights_out[...] = weights[...]
    duals_out[...] = duals[...]
    objectives_out[...] = objectives[...]


def on_device(sizes, inputs, frequencies, phases, targets, block_order):
    nx, nz, ny, nc = sizes
    rows, raw = inputs.shape
    width = frequencies.shape[1]
    held = nc * BLOCK
    members = ny * nx
    share = width // nx
    vmem = pl.BlockSpec(memory_space=pltpu.VMEM)
    dma = pltpu.SemaphoreType.DMA
    scratch = [
        pltpu.VMEM((raw, rows), BF16),
        pltpu.VMEM((1, rows), F32),
        pltpu.VMEM((1, rows), jnp.int32),
        pltpu.VMEM((held, 128), BF16),
        pltpu.VMEM((rows, held), BF16),
        pltpu.VMEM((ny, 128, width), BF16),
        pltpu.VMEM((ny, 1, width), F32),
        pltpu.VMEM((held, ny * width), BF16),
        pltpu.VMEM((nc, BLOCK, BLOCK), F32),
        pltpu.VMEM((BLOCK, BLOCK), F32),
        pltpu.VMEM((2 * BLOCK, BLOCK), F32),
        pltpu.VMEM((nc, BLOCK, BLOCK), F32),
        pltpu.VMEM((held, 128), F32),
        pltpu.VMEM((held, 128), F32),
        pltpu.VMEM((ROUNDS, 1, held), F32),
        pltpu.VMEM((ROUNDS, 1, held), F32),
        pltpu.VMEM((ROUNDS, members, 1, share), F32),
        pltpu.VMEM((ROUNDS, members, 1, share), F32),
        pltpu.VMEM((ROUNDS, nz, 1, share), F32),
        pltpu.VMEM((ROUNDS, members, 1, share), F32),
        pltpu.VMEM((ROUNDS, nc, 1, held), F32),
        pltpu.VMEM((1, nc, 1, 128), F32),
        pltpu.VMEM((1, ny, 1, rows), F32),
        pltpu.VMEM((1, members, 2, 128), F32),
        pltpu.VMEM((1, nz, 2, 128), F32),
        dma((5,)),
        dma((ny, PIECES)),
        dma((ny,)),
        dma((1,)),
        dma((nc,)),
        dma((ROUNDS, members)),
        dma((ROUNDS, nz)),
        dma((ROUNDS, members)),
        dma((ROUNDS, nc)),
        dma((1, nc)),
        dma((1, ny)),
        dma((1, members)),
        dma((1, nz)),
        dma((PIECES,)),
        dma((PIECES,)),
        dma((PIECES,)),
        dma((ny,)),
        dma((3,)),
        dma((members,)),
        dma((nz,)),
        dma((members,)),
        dma((1,)),
        dma((ny,)),
        dma((members,)),
        dma((nz,)),
    ]
    shapes = (
        jax.ShapeDtypeStruct((1, width), F32),
        jax.ShapeDtypeStruct((1, rows), F32),
        jax.ShapeDtypeStruct((2, ROUNDS), F32),
    )
    results = pl.pallas_call(
        functools.partial(kernel, sizes),
        out_shape=shapes,
        in_specs=[pl.BlockSpec(memory_space=pl.ANY)] * 5,
        out_specs=(vmem, vmem, vmem),
        scratch_shapes=scratch,
        compiler_params=pltpu.CompilerParams(
            collective_id=0, has_side_effects=True, vmem_limit_bytes=60 * 1024 * 1024
        ),
        name="cocoa",
    )(
        inputs.T,
        frequencies,
        phases.reshape(1, width),
        targets.reshape(1, rows),
        block_order.reshape(1, rows),
    )
    weights, duals, objectives = pl.pallas_call(
        copied,
        out_shape=shapes,
        in_specs=[vmem] * 3,
        out_specs=(vmem, vmem, vmem),
        name="results",
    )(*results)
    return weights.reshape(width), duals.reshape(rows), objectives.T


def solution(mesh):
    devices = mesh.devices
    samp, feat = mesh.shape["samp"], mesh.shape["feat"]
    nc = 2
    ny = feat // nc
    nx = math.gcd(samp, 4)
    nz = samp // nx
    torus = Mesh(devices.reshape(nx, nz, ny, nc), ("x", "z", "y", "core"))
    samp_axes, feat_axes = ("x", "z"), ("y", "core")
    in_specs = (
        P(samp_axes, None),
        P(None, feat_axes),
        P(feat_axes),
        P(samp_axes),
        P(samp_axes),
    )
    out_specs = (P(feat_axes), P(samp_axes), P())
    return jax.shard_map(
        functools.partial(on_device, (nx, nz, ny, nc)),
        mesh=torus,
        in_specs=in_specs,
        out_specs=out_specs,
        check_vma=False,
    )
```
